32 devices in a mesh: ctx: 4 (over y, x), fsdp: 8 (over z, core).
Axes of the slice: x: 2, y: 2, z: 4, core: 2. Of those that a mesh axis runs over, the one named last changes fastest.
Arguments:
- query_a: bfloat16 [8, 512, 2048], P('fsdp', 'ctx'), may hold values from -64 to 64
- key_a: bfloat16 [8, 512, 256], P('fsdp', 'ctx'), may hold values from -8 to 8
- value_a: bfloat16 [8, 512, 256], P('fsdp', 'ctx'), may hold values from -6 to 6
- resid_in: bfloat16 [8, 512, 1440], P('fsdp', 'ctx'), may hold values from -6 to 6
- doc_lengths: int32 [8, 6], P('fsdp'), may hold values from 1 to 384, 512 in all within a row
- w_out: bfloat16 [2048, 1440], P('fsdp'), may hold values from -0.125 to 0.125
- w_qkv: bfloat16 [1440, 2560], P('fsdp'), may hold values from -8 to 8
- grad_out: bfloat16 [8, 512, 2048], P('fsdp', 'ctx'), may hold values from -6 to 6
- grad_resid: bfloat16 [8, 512, 1440], P('fsdp', 'ctx'), may hold values from -8 to 8
Outputs:
- banded_out: bfloat16 [8, 512, 2048], P('fsdp', 'ctx')
- grad_input: bfloat16 [8, 512, 1440], P('fsdp', 'ctx')
- grad_query: bfloat16 [8, 512, 2048], P('fsdp', 'ctx')
- grad_key: bfloat16 [8, 512, 256], P('fsdp', 'ctx')
- grad_value: bfloat16 [8, 512, 256], P('fsdp', 'ctx')
- grad_w_out: float32 [2048, 1440], P('fsdp')
- grad_w_qkv: float32 [1440, 2560], P('fsdp')
The draws below stay inside these ranges and needn't reach their ends.
Inputs may be any that keep to these rules, and one draw needn't show every extreme that they name: `doc_lengths`: the lengths of a sequence sum to 512, and one document has 384 positions.
All inputs are finite; a program needn't handle non-finite values.
Results may differ from the reference program's by a relative error of at most 0.03.
Values may be sent and summed in bfloat16 or wider, within the bound.
A program may use at most 128 MiB of HBM per device.

```python
import math
import jax
import jax.numpy as jnp
import numpy as np
from jax import lax

H = 32
KV = 4
DH = 64
D = 1440
BAND = 128
DOCS = 6
TOK_DEV = 128
SEQ = 512
SEQS = 8
N_CTX = 4


def drawn_pair(key):
    key_query, key_keys = jax.random.split(key, 2)
    shape_query = (SEQS, SEQ, H * DH)
    shape_keys = (SEQS, SEQ, KV * DH)
    query = jax.random.truncated_normal(key_query, -4.0, 4.0, shape_query, jnp.float32)
    keys = jax.random.truncated_normal(key_keys, -4.0, 4.0, shape_keys, jnp.float32)
    return (query.astype(jnp.bfloat16), keys.astype(jnp.bfloat16))


def draw_query_a(key, part):
    return drawn_pair(jax.random.fold_in(key, 7))[0]


def draw_key_a(key, part):
    return drawn_pair(jax.random.fold_in(key, 7))[1]


def draw_w_qkv(key, part):
    width = (H + 2 * KV) * DH
    matrix = jax.random.truncated_normal(key, -4.0, 4.0, (D, width), jnp.float32) * D ** (-0.5)
    return matrix.astype(jnp.bfloat16)


def draw_grad_resid(key, part):
    key_common, key_rough = jax.random.split(jax.random.fold_in(key, 11))
    common = 0.8 * jax.random.normal(key_common, (SEQS, 1, D), jnp.float32)
    rough = jax.random.normal(key_rough, (SEQS, SEQ, D), jnp.float32)
    return jnp.clip(common + rough, -7.5, 7.5).astype(jnp.bfloat16)


def level_of(key, dims, cuts, low, largest):
    loudness, own = 1.0, jax.random.fold_in(key, 6)
    for position, blocks in cuts:
        draws = jnp.exp(jax.random.uniform(jax.random.fold_in(own, position), (blocks,), jnp.float32, low / len(cuts), largest / len(cuts)))
        loudness = loudness * jnp.repeat(draws, dims[position] // blocks).reshape([-1 if axis == position else 1 for axis in range(len(dims))])
    return loudness


def length_profile(number_of, total, bound, lean):
    loads = [(1 << 20) // math.isqrt(standing ** lean) + 1 for standing in range(2, number_of + 1)]
    surplus, counts = total - bound - (number_of - 1), [1] * (number_of - 1)
    while surplus > 0:
        candidates = [i for i in range(number_of - 1) if counts[i] < bound]
        whole, remaining = sum([loads[i] for i in candidates]), surplus
        for i in candidates:
            extra = min(bound - counts[i], max(1, remaining * loads[i] // whole), surplus)
            counts[i] = counts[i] + extra
            surplus = surplus - extra
    return np.array([bound] + counts)


def ragged(own_key, amount, total, most, skew):
    if amount == 2:
        one = jax.random.randint(own_key, (), max(1, total - most), min(most, total - 1) + 1)
        return jnp.stack([one, total - one])
    sizes = jnp.asarray(length_profile(amount, total, most, skew), jnp.int32)
    twos = (amount - 1) // 2
    source_of, receiver = sizes[1:1 + 2 * twos:2], sizes[2:2 + 2 * twos:2]
    margin = jnp.minimum(source_of - 1, most - receiver)
    shifted = jax.random.randint(jax.random.fold_in(own_key, 1), (twos,), 0, 1 << 20) % (margin + 1)
    sizes = sizes.at[1:1 + 2 * twos:2].set(source_of - shifted).at[2:2 + 2 * twos:2].set(receiver + shifted)
    return sizes[jax.random.permutation(jax.random.fold_in(own_key, 2), amount)]


def normal_values(stream_key, extent, deviation, bound, cuts=(), kind=jnp.bfloat16):
    values = jax.random.normal(stream_key, extent, jnp.float32) * deviation
    if len(cuts) > 0:
        values = level_of(stream_key, extent, cuts, -0.22, 0.18) * values
    return jnp.clip(values, min=-bound, max=bound).astype(kind)


def setup_inputs(seed: int = 0) -> dict:
    key_of = jax.random.split(jax.random.key(seed), 10)
    query_a = draw_query_a(jax.random.fold_in(key_of[9], 71), 0)
    key_a = draw_key_a(jax.random.fold_in(key_of[9], 71), 0)
    value_a = normal_values(key_of[2], (SEQS, SEQ, KV * DH), 1.0, 6.0, ((0, 8), (1, 4)))
    resid_in = normal_values(key_of[3], (SEQS, SEQ, D), 1.0, 6.0, ((0, 8), (1, 4)))
    doc_lengths = jax.vmap(lambda own: ragged(own, DOCS, SEQ, 3 * SEQ // 4, 2))(jax.random.split(key_of[4], SEQS)).reshape((SEQS, DOCS)).astype(jnp.int32)
    w_out = normal_values(key_of[5], (H * DH, D), (H * DH) ** -0.5, 0.125, ((0, 8),))
    w_qkv = draw_w_qkv(jax.random.fold_in(key_of[9], 71), 0)
    grad_out = normal_values(key_of[7], (SEQS, SEQ, H * DH), 1.0, 6.0, ((0, 8), (1, 4)))
    grad_resid = draw_grad_resid(jax.random.fold_in(key_of[9], 71), 0)
    return dict(query_a=query_a, key_a=key_a, value_a=value_a, resid_in=resid_in, doc_lengths=doc_lengths, w_out=w_out, w_qkv=w_qkv, grad_out=grad_out, grad_resid=grad_resid)


MASKED = -1e+30
EPSILON = 1e-05

def doc_index(lengths):
    ends = jnp.cumsum(lengths)
    places = jnp.arange(SEQ, dtype=jnp.int32)
    return lax.optimization_barrier(jnp.sum((places[:, None] >= ends[None, :]).astype(jnp.int32), axis=1))

def allowed_pairs(documents, reach):
    places = jnp.arange(SEQ, dtype=jnp.int32)
    behind = places[:, None] - places[None, :]
    same_doc = documents[:, None] == documents[None, :]
    return same_doc & (behind >= 0) & (behind < reach)

def query_heads(rows):
    return rows.reshape(SEQ, KV, H // KV, DH).transpose(1, 2, 0, 3)

def pair_heads(rows):
    return rows.reshape(SEQ, KV, DH).transpose(1, 0, 2)

def merge_query(heads):
    return heads.transpose(2, 0, 1, 3).reshape(SEQ, H * DH)

def merge_pair(heads):
    return heads.transpose(1, 0, 2).reshape(SEQ, KV * DH)

def attention_weights(query_group, key_head, allowed):
    scores = jnp.einsum('gid,jd->gij', query_group.astype(jnp.float32), key_head.astype(jnp.float32)) * DH ** (-0.5)
    scores = jnp.where(allowed, scores, MASKED)
    row_max = lax.optimization_barrier(jnp.max(scores, axis=-1, keepdims=True))
    log_total = row_max + jnp.log(lax.optimization_barrier(jnp.sum(jnp.where(allowed, jnp.exp(scores - row_max), 0.0), axis=-1, keepdims=True)))
    return jnp.where(allowed, jnp.exp(scores - log_total), 0.0)

def attend(query, keys, values, allowed):

    def one_head(items):
        query_group, key_head, value_head = items
        weights = attention_weights(query_group, key_head, allowed).astype(jnp.bfloat16)
        summed = jnp.einsum('gij,jd->gid', weights.astype(jnp.float32), value_head.astype(jnp.float32))
        return summed.astype(jnp.bfloat16)
    return merge_query(lax.map(one_head, (query_heads(query), pair_heads(keys), pair_heads(values))))

def attend_back(query, keys, values, output, grad, allowed):

    def one_head(items):
        query_group, key_head, value_head, out_group, grad_group = items
        weights = attention_weights(query_group, key_head, allowed)
        weights_bf = weights.astype(jnp.bfloat16)
        grad_weights = jnp.einsum('gid,jd->gij', grad_group.astype(jnp.float32), value_head.astype(jnp.float32))
        correction = lax.optimization_barrier(jnp.sum(grad_group.astype(jnp.float32) * out_group.astype(jnp.float32), axis=-1, keepdims=True))
        grad_scores = (weights * (grad_weights - correction)).astype(jnp.bfloat16)
        grad_q = jnp.einsum('gij,jd->gid', grad_scores.astype(jnp.float32), key_head.astype(jnp.float32)) * DH ** (-0.5)
        grad_k = jnp.einsum('gij,gid->jd', grad_scores.astype(jnp.float32), query_group.astype(jnp.float32)) * DH ** (-0.5)
        grad_v = jnp.einsum('gij,gid->jd', weights_bf.astype(jnp.float32), grad_group.astype(jnp.float32))
        return (grad_q.astype(jnp.bfloat16), grad_k.astype(jnp.bfloat16), grad_v.astype(jnp.bfloat16))
    items = (query_heads(query), pair_heads(keys), pair_heads(values), query_heads(output), query_heads(grad))
    grad_q, grad_k, grad_v = lax.map(one_head, items)
    return (merge_query(grad_q), merge_pair(grad_k), merge_pair(grad_v))

def block_terms(left, right, total):
    left_blocks = left.reshape(N_CTX, TOK_DEV, left.shape[1])
    right_blocks = right.reshape(N_CTX, TOK_DEV, right.shape[1])

    def add_block(acc, pieces):
        left_piece, right_piece = pieces
        term = jnp.dot(left_piece.T, right_piece, preferred_element_type=jnp.float32).astype(jnp.bfloat16)
        term = lax.optimization_barrier(term)
        return (acc + term.astype(jnp.float32), None)
    total, unused = lax.scan(add_block, total, (left_blocks, right_blocks))
    return total

def reference(query_a, key_a, value_a, resid_in, doc_lengths, w_out, w_qkv, grad_out, grad_resid):

    def one_sequence(carry, items):
        sum_out, sum_qkv = carry
        query, keys, values, resid, lengths, grad_o, grad_r = items
        documents = doc_index(lengths)
        full_allowed = allowed_pairs(documents, SEQ)
        band_allowed = allowed_pairs(documents, BAND)
        attended = attend(query, keys, values, full_allowed)
        resid_mid = (resid.astype(jnp.float32) + jnp.dot(attended, w_out, preferred_element_type=jnp.float32)).astype(jnp.bfloat16)
        resid_f = resid_mid.astype(jnp.float32)
        inverse_rms = lax.rsqrt(lax.optimization_barrier(jnp.mean(resid_f * resid_f, axis=-1, keepdims=True)) + EPSILON)
        normed = resid_f * inverse_rms
        normed_bf = normed.astype(jnp.bfloat16)
        projected = jnp.dot(normed_bf, w_qkv, preferred_element_type=jnp.float32).astype(jnp.bfloat16)
        query_b = projected[:, :H * DH]
        key_b = projected[:, H * DH:H * DH + KV * DH]
        value_b = projected[:, H * DH + KV * DH:]
        banded = attend(query_b, key_b, value_b, band_allowed)
        grad_qb, grad_kb, grad_vb = attend_back(query_b, key_b, value_b, banded, grad_o, band_allowed)
        grad_proj = jnp.concatenate([grad_qb, grad_kb, grad_vb], axis=1)
        grad_normed = jnp.dot(grad_proj, w_qkv.T, preferred_element_type=jnp.float32)
        middle = lax.optimization_barrier(jnp.mean(grad_normed * normed, axis=-1, keepdims=True))
        grad_mid = (grad_r.astype(jnp.float32) + inverse_rms * (grad_normed - normed * middle)).astype(jnp.bfloat16)
        grad_attended = jnp.dot(grad_mid, w_out.T, preferred_element_type=jnp.float32).astype(jnp.bfloat16)
        grad_q, grad_k, grad_v = attend_back(query, keys, values, attended, grad_attended, full_allowed)
        sum_out = block_terms(attended, grad_mid, sum_out)
        sum_qkv = block_terms(normed_bf, grad_proj, sum_qkv)
        return ((sum_out, sum_qkv), (banded, grad_mid, grad_q, grad_k, grad_v))
    items = (query_a, key_a, value_a, resid_in, doc_lengths, grad_out, grad_resid)
    start = (jnp.zeros(w_out.shape, jnp.float32), jnp.zeros(w_qkv.shape, jnp.float32))
    (grad_w_out, grad_w_qkv), outputs = lax.scan(one_sequence, start, items)
    banded_out, grad_input, grad_query, grad_key, grad_value = outputs
    return (banded_out, grad_input, grad_query, grad_key, grad_value, grad_w_out, grad_w_qkv)
```

```python
import functools

import jax
import jax.numpy as jnp
from jax import lax
from jax.experimental import pallas as pl
from jax.experimental.pallas import tpu as pltpu
from jax.sharding import PartitionSpec as P

H = 32
KV = 4
DH = 64
BAND = 128


MASKED = -1e30
EPSILON = 1e-05


def from_behind(value, axis, steps):
    count = lax.axis_size(axis)
    leading, last = (max(0, -steps), min(count, count - steps))
    return lax.ppermute(value, axis, [(source, source + steps) for source in range(leading, last)])


def doc_table(lengths, seq_len):
    ends = jnp.cumsum(lengths)
    places = jnp.arange(seq_len, dtype=jnp.int32)
    before = places[:, None] >= ends[None, :]
    return jnp.sum(before.astype(jnp.int32), axis=1)


def attend_kernel(with_output, with_grads, *refs):
    refs = list(refs)
    allowed_ref, q_ref, k_ref, v_ref, v_t_ref = refs[:5]
    del refs[:5]
    if with_grads:
        k_t_ref, g_ref = refs[:2]
        del refs[:2]
    o_ref = refs.pop(0)
    if with_grads:
        dq_ref, dk_ref, dv_ref = refs
    allowed = allowed_ref[...] > 0.0
    keys, values, values_t = (k_ref[0], v_ref[0], v_t_ref[...])
    dk = jnp.zeros(keys.shape, jnp.float32)
    dv = jnp.zeros(keys.shape, jnp.float32)
    by_last = (((1,), (1,)), ((), ()))
    for head in range(H // KV):
        rows = slice(head * DH, (head + 1) * DH)
        query = q_ref[rows, :]
        scores = jnp.dot(keys, query, preferred_element_type=jnp.float32) * DH ** (-0.5)
        scores = jnp.where(allowed, scores, MASKED)
        row_max = jnp.max(scores, axis=0, keepdims=True)
        log_total = row_max + jnp.log(
            jnp.sum(jnp.exp(scores - row_max), axis=0, keepdims=True)
        )
        weights = jnp.where(allowed, jnp.exp(scores - log_total), 0.0)
        weights_bf = weights.astype(jnp.bfloat16)
        if with_output:
            output = jnp.dot(values_t, weights_bf, preferred_element_type=jnp.float32)
            output = output.astype(jnp.bfloat16)
            o_ref[rows, :] = output
        else:
            output = o_ref[rows, :]
        if with_grads:
            grad = g_ref[rows, :]
            correction = jnp.sum(
                grad.astype(jnp.float32) * output.astype(jnp.float32), axis=0, keepdims=True
            )
            grad_weights = jnp.dot(values, grad, preferred_element_type=jnp.float32)
            grad_scores = (weights * (grad_weights - correction)).astype(jnp.bfloat16)
            grad_q = jnp.dot(k_t_ref[...], grad_scores, preferred_element_type=jnp.float32)
            dq_ref[rows, :] = (grad_q * DH ** (-0.5)).astype(jnp.bfloat16)
            dk += lax.dot_general(grad_scores, query, by_last, preferred_element_type=jnp.float32)
            dv += lax.dot_general(weights_bf, grad, by_last, preferred_element_type=jnp.float32)
    if with_grads:
        dk_ref[0] = dk
        dv_ref[0] = dv


def by_head(rows):
    return rows.reshape(rows.shape[0], KV, DH).transpose(1, 0, 2)


def from_heads(heads):
    return heads.transpose(1, 0, 2).reshape(heads.shape[1], KV * DH)


def attend(allowed_t, query_t, keys, values, output_t=None, grad_t=None):
    columns, rows = allowed_t.shape
    with_output, with_grads = (output_t is None, grad_t is not None)
    group = pl.BlockSpec((query_t.shape[0] // KV, rows), lambda g: (g, 0))
    key_rows = pl.BlockSpec((1, columns, DH), lambda g: (g, 0, 0))
    key_columns = pl.BlockSpec((DH, columns), lambda g: (g, 0))
    args = [allowed_t, query_t, by_head(keys), by_head(values), values.T]
    in_specs = [pl.BlockSpec((columns, rows), lambda g: (0, 0)), group]
    in_specs += [key_rows, key_rows, key_columns]
    out_shape, out_specs = ([], [])
    wide = jax.ShapeDtypeStruct(query_t.shape, jnp.bfloat16)
    narrow = jax.ShapeDtypeStruct((KV, columns, DH), jnp.float32)
    if with_grads:
        args += [keys.T, grad_t]
        in_specs += [key_columns, group]
    if with_output:
        out_shape.append(wide)
        out_specs.append(group)
    else:
        args.append(output_t)
        in_specs.append(group)
    if with_grads:
        out_shape += [wide, narrow, narrow]
        out_specs += [group, key_rows, key_rows]
    return pl.pallas_call(
        functools.partial(attend_kernel, with_output, with_grads),
        grid=(KV,),
        out_shape=tuple(out_shape),
        in_specs=in_specs,
        out_specs=tuple(out_specs),
    )(*args)


MESH = pl.DeviceIdType.MESH


def remote(src, dst, send_sem, recv_sem, ctx, fsdp):
    return pltpu.make_async_remote_copy(
        src_ref=src,
        dst_ref=dst,
        send_sem=send_sem,
        recv_sem=recv_sem,
        device_id={"ctx": ctx, "fsdp": fsdp},
        device_id_type=MESH,
    )


def place():
    return (lax.axis_index("ctx"), lax.axis_index("fsdp"))


def shard_at(z, core, planes, offset):
    return 2 * lax.rem(z + offset, planes) + core


def greet(planes):
    c, f = place()
    z, core = (f // 2, lax.rem(f, 2))
    barrier = pltpu.get_barrier_semaphore()
    peers = [(c ^ 1, f), (c ^ 2, f), (c ^ 3, f), (c, f ^ 1)]
    peers += [(c, shard_at(z, core, planes, d)) for d in range(1, planes)]
    for ctx, fsdp in peers:
        pl.semaphore_signal(
            barrier, inc=1, device_id={"ctx": ctx, "fsdp": fsdp}, device_id_type=MESH
        )
    pl.semaphore_wait(barrier, len(peers))


def quarter_of(ref, weight, quarter):
    if weight == 0:
        size = ref.shape[0] // 4
        return ref.at[pl.ds(pl.multiple_of(quarter * size, 16), size), :]
    size = ref.shape[1] // 4
    return ref.at[:, pl.ds(pl.multiple_of(quarter * size, 128), size)]


def by_distance(planes):
    order = []
    for step in range(1, planes // 2 + 1):
        for d in (step, planes - step):
            if d not in order:
                order.append(d)
    return order


def gather_kernel(
    planes, wo, wq, kv, go, gq, gkv, send, recv_z, recv_x, recv_y, recv_d, recv_p, recv_kv, local
):
    c, f = place()
    z, core = (f // 2, lax.rem(f, 2))
    mine, full = ((wo, wq), (go, gq))
    rows = kv.shape[0]
    owns = [
        pltpu.make_async_copy(kv, gkv.at[pl.ds(pl.multiple_of(c * rows, 128), rows)], local),
        pltpu.make_async_copy(wo, go.at[f], local),
        pltpu.make_async_copy(wq, gq.at[f], local),
    ]
    for copy in owns:
        copy.start()
    greet(planes)
    started = []

    def push(*args):
        copy = remote(*args)
        copy.start()
        started.append(copy)

    def piece(weight, shard, quarter):
        return quarter_of(full[weight].at[shard], weight, quarter)

    def arrive(ref, sem):
        remote(ref, ref, send, sem, c ^ 1, f).wait_recv()

    kv_place = gkv.at[pl.ds(pl.multiple_of(c * rows, 128), rows)]
    for i, bit in enumerate((1, 2, 3)):
        push(kv, kv_place, send, recv_kv.at[i], c ^ bit, f)
    order = by_distance(planes)
    for weight in (0, 1):
        for d in order:
            push(
                quarter_of(mine[weight], weight, c),
                piece(weight, f, c),
                send,
                recv_z.at[weight, d],
                c,
                shard_at(z, core, planes, d),
            )
        push(mine[weight], full[weight].at[f], send, recv_p.at[weight, 0, 0], c, f ^ 1)
    steps = [(weight, d) for weight in (0, 1) for d in order]

    def to_partner(weight, d, shard, slot):
        part = piece(weight, shard, c ^ slot)
        push(part, part, send, recv_p.at[weight, d, slot], c, f ^ 1)

    def first(weight, d):
        shard = shard_at(z, core, planes, planes - d)
        part = piece(weight, shard, c)
        arrive(part, recv_z.at[weight, d])
        push(part, part, send, recv_x.at[weight, d], c ^ 1, f)
        push(part, part, send, recv_y.at[weight, d], c ^ 2, f)
        to_partner(weight, d, shard, 0)

    def second(weight, d):
        shard = shard_at(z, core, planes, planes - d)
        arrive(piece(weight, shard, c ^ 1), recv_x.at[weight, d])
        arrive(piece(weight, shard, c ^ 2), recv_y.at[weight, d])
        bit = jnp.where(core == weight, 1, 2)
        part = piece(weight, shard, c ^ bit)
        push(part, part, send, recv_d.at[weight, d], c ^ (3 - bit), f)
        to_partner(weight, d, shard, 1)
        to_partner(weight, d, shard, 2)

    def third(weight, d):
        shard = shard_at(z, core, planes, planes - d)
        arrive(piece(weight, shard, c ^ 3), recv_d.at[weight, d])
        to_partner(weight, d, shard, 3)

    count = len(steps)
    for i in range(count + 2):
        if i < count:
            first(*steps[i])
        if 0 <= i - 1 < count:
            second(*steps[i - 1])
        if 0 <= i - 2 < count:
            third(*steps[i - 2])
    for weight in (0, 1):
        arrive(full[weight].at[f ^ 1], recv_p.at[weight, 0, 0])
        for d in order:
            shard = shard_at(z, core, planes, planes - d) ^ 1
            for slot in range(4):
                arrive(piece(weight, shard, c ^ slot), recv_p.at[weight, d, slot])
    for i in range(3):
        arrive(kv_place, recv_kv.at[i])
    for copy in started:
        copy.wait_send()
    for copy in owns:
        copy.wait()


def gather_weights(w_out, w_qkv, kv):
    count = lax.axis_size("fsdp")
    planes = count // 2
    dma = pltpu.SemaphoreType.DMA
    anywhere = pl.BlockSpec(memory_space=pl.ANY)
    return pl.pallas_call(
        functools.partial(gather_kernel, planes),
        out_shape=(
            jax.ShapeDtypeStruct((count,) + w_out.shape, w_out.dtype),
            jax.ShapeDtypeStruct((count,) + w_qkv.shape, w_qkv.dtype),
            jax.ShapeDtypeStruct((4 * kv.shape[0], kv.shape[1]), kv.dtype),
        ),
        in_specs=[anywhere] * 3,
        out_specs=(anywhere,) * 3,
        scratch_shapes=[
            dma,
            dma((2, planes)),
            dma((2, planes)),
            dma((2, planes)),
            dma((2, planes)),
            dma((2, planes, 4)),
            dma((3,)),
            dma,
        ],
        compiler_params=pltpu.CompilerParams(collective_id=0, has_side_effects=True),
    )(w_out, w_qkv, kv)


def reduce_kernel(
    planes,
    att_t,
    norm_t,
    grad_mid,
    grad_proj,
    kv_sums,
    out_o,
    out_q,
    out_kv,
    a_o,
    a_q,
    s_o,
    s_q,
    p_o,
    p_q,
    r1_o,
    r1_q,
    r2_o,
    r2_q,
    rz_o,
    rz_q,
    from_kv,
    send,
    recv_p,
    recv_1,
    recv_2,
    recv_z,
    recv_f,
    recv_kv,
):
    c, f = place()
    z, core = (f // 2, lax.rem(f, 2))
    greet(planes)
    own, sent, from_p, from_1, from_2, from_z, result = (
        (a_o, a_q),
        (s_o, s_q),
        (p_o, p_q),
        (r1_o, r1_q),
        (r2_o, r2_q),
        (rz_o, rz_q),
        (out_o, out_q),
    )
    started = []

    def push(*args):
        copy = remote(*args)
        copy.start()
        started.append(copy)

    def arrive(ref, sem):
        remote(ref, ref, send, sem, c ^ 1, f).wait_recv()

    def term(weight, shard):
        if weight == 0:
            size = a_o.shape[1]
            left = att_t[pl.ds(pl.multiple_of(shard * size, size), size), :]
            right = grad_mid[...]
        else:
            left = norm_t[shard]
            right = grad_proj[...]
        return jnp.dot(left, right, preferred_element_type=jnp.float32).astype(jnp.bfloat16)

    def added(first, second):
        return (first.astype(jnp.float32) + second.astype(jnp.float32)).astype(jnp.bfloat16)

    rows = out_kv.shape[0]

    def kv_rows(index):
        return kv_sums.at[pl.ds(pl.multiple_of(index * rows, rows), rows), :]

    for slot in (3, 1, 2):
        push(
            kv_rows(c ^ slot), from_kv.at[slot], send, recv_kv.at[slot], c ^ slot, f
        )
    order = by_distance(planes)[::-1] + [0]
    steps = [(weight, d) for d in order for weight in (1, 0)]

    def bits(weight):
        bit = jnp.where(core == weight, 1, 2)
        return (bit, 3 - bit)

    def produce(weight, d):
        shard = shard_at(z, core, planes, d)
        sent[weight][d] = term(weight, shard ^ 1)
        push(sent[weight].at[d], from_p[weight].at[d], send, recv_p.at[weight, d], c, f ^ 1)
        own[weight][d] = term(weight, shard)

    def chip_sum(weight, d):
        arrive(from_p[weight].at[d], recv_p.at[weight, d])
        own[weight][d] = added(own[weight][d], from_p[weight][d])
        bit, other = bits(weight)
        for slot, quarter in ((1, c ^ 3), (0, c ^ bit)):
            push(
                quarter_of(own[weight].at[d], weight, quarter),
                from_1[weight].at[d, slot],
                send,
                recv_1.at[weight, d, slot],
                c ^ bit,
                f,
            )

    def pair_sum(weight, d):
        bit, other = bits(weight)
        for slot, quarter in ((1, c ^ other), (0, c)):
            arrive(from_1[weight].at[d, slot], recv_1.at[weight, d, slot])
            part = quarter_of(own[weight].at[d], weight, quarter)
            part[...] = added(part[...], from_1[weight][d, slot])
            if slot == 1:
                push(part, from_2[weight].at[d], send, recv_2.at[weight, d], c ^ other, f)

    def plane_sum(weight, d):
        arrive(from_2[weight].at[d], recv_2.at[weight, d])
        part = quarter_of(own[weight].at[d], weight, c)
        part[...] = added(part[...], from_2[weight][d])
        if d:
            push(
                part,
                from_z[weight].at[d],
                send,
                recv_z.at[weight, d],
                c,
                shard_at(z, core, planes, d),
            )

    def finish(weight):
        part = quarter_of(own[weight].at[0], weight, c)
        total = part[...].astype(jnp.float32)
        for d in range(1, planes):
            arrive(from_z[weight].at[d], recv_z.at[weight, d])
            total = total + from_z[weight][d].astype(jnp.float32)
        place_c = quarter_of(result[weight], weight, c)
        place_c[...] = total.astype(jnp.bfloat16)
        for slot in (3, 1, 2):
            push(place_c, place_c, send, recv_f.at[weight, slot], c ^ slot, f)

    stages = (produce, chip_sum, pair_sum, plane_sum)
    lags = (0, 2, 4, 6)
    count = len(steps)
    for i in range(count + lags[-1]):
        for stage, lag in zip(stages, lags):
            if 0 <= i - lag < count:
                stage(*steps[i - lag])
    kv_total = kv_rows(c)[...].astype(jnp.float32)
    for slot in (1, 2, 3):
        arrive(from_kv.at[slot], recv_kv.at[slot])
        kv_total += from_kv[slot].astype(jnp.float32)
    out_kv[...] = kv_total
    for weight in (1, 0):
        finish(weight)
    for weight in (1, 0):
        for slot in (3, 1, 2):
            arrive(quarter_of(result[weight], weight, c ^ slot), recv_f.at[weight, slot])
    for copy in started:
        copy.wait_send()


def reduce_weights(att_t, norm_t, grad_mid, grad_proj, kv_sums):
    count = lax.axis_size("fsdp")
    planes = count // 2
    dma = pltpu.SemaphoreType.DMA
    in_vmem = pl.BlockSpec(memory_space=pltpu.VMEM)
    bf = jnp.bfloat16
    o_shape = (att_t.shape[0] // count, grad_mid.shape[1])
    q_shape = (norm_t.shape[1], grad_proj.shape[1])
    o_part = (o_shape[0] // 4, o_shape[1])
    q_part = (q_shape[0], q_shape[1] // 4)
    scratch = []
    for lead, shapes in (
        ((planes,), (o_shape, q_shape)),
        ((planes,), (o_shape, q_shape)),
        ((planes,), (o_shape, q_shape)),
        ((planes, 2), (o_part, q_part)),
        ((planes,), (o_part, q_part)),
        ((planes,), (o_part, q_part)),
    ):
        scratch += [pltpu.VMEM(lead + shape, bf) for shape in shapes]
    kv_shape = (kv_sums.shape[0] // 4, kv_sums.shape[1])
    scratch.append(pltpu.VMEM((4,) + kv_shape, bf))
    return pl.pallas_call(
        functools.partial(reduce_kernel, planes),
        out_shape=(
            jax.ShapeDtypeStruct(o_shape, bf),
            jax.ShapeDtypeStruct(q_shape, bf),
            jax.ShapeDtypeStruct(kv_shape, jnp.float32),
        ),
        in_specs=[in_vmem] * 5,
        out_specs=(in_vmem,) * 3,
        scratch_shapes=scratch
        + [
            dma,
            dma((2, planes)),
            dma((2, planes, 2)),
            dma((2, planes)),
            dma((2, planes)),
            dma((2, 4)),
            dma((4,)),
        ],
        compiler_params=pltpu.CompilerParams(
            collective_id=1, has_side_effects=True, vmem_limit_bytes=60 * 2**20
        ),
    )(att_t, norm_t, grad_mid, grad_proj, kv_sums)


def mega_kernel(
    planes,
    lens,
    q_in,
    k_in,
    v_in,
    resid_in,
    wo_in,
    wq_in,
    go_in,
    gr_in,
    out_b,
    out_gm,
    out_dq,
    out_dk,
    out_dv,
    res_o,
    res_q,
    q_v,
    resid_v,
    wo_v,
    go_v,
    gr_v,
    w_o,
    w_q,
    kv,
    kh,
    vh,
    kv_t,
    qp,
    gp,
    bias,
    bias_b,
    probs,
    o_p,
    att_t,
    att8,
    attq,
    acc,
    acc_p,
    normed,
    inv,
    xb,
    nt,
    kvx,
    khb,
    vhb,
    kvx_t,
    qb,
    ob_t,
    dqb_t,
    dkv_b,
    tail,
    head,
    gp4,
    gpq,
    gn,
    gm,
    dkv_t,
    kvs,
    kvr,
    s_q,
    p_q,
    z_q,
    t_q,
    s_o,
    p_o,
    z_o,
    t_o,
    local,
    send,
    recv_kv,
    recv_z,
    recv_x,
    recv_y,
    recv_d,
    recv_p,
    recv_att,
    recv_nt,
    recv_halo,
    recv_gp,
    recv_gm,
    recv_kvs,
    recv_rp,
    recv_rz,
    recv_f,
):
    f32, bf = (jnp.float32, jnp.bfloat16)
    c, f = place()
    z, core = (f // 2, lax.rem(f, 2))
    toks = q_in.shape[0]
    kvd = k_in.shape[1]
    shards = 2 * planes
    groups = kh.shape[0]
    pairs = qp.shape[0]
    per_group = pairs // groups
    per_shard = att_t.shape[1]
    scale = DH ** (-0.5)
    full = (w_o, w_q)
    by_last = (((1,), (1,)), ((), ()))
    started = []

    def push(*args):
        copy = remote(*args)
        copy.start()
        started.append(copy)

    def arrive(ref, sem):
        remote(ref, ref, send, sem, c ^ 1, f).wait_recv()

    def dot(a, b):
        return jnp.dot(a, b, preferred_element_type=f32)

    def dot_nt(a, b):
        return lax.dot_general(a, b, by_last, preferred_element_type=f32)

    names = ((wo_in, wo_v), (q_in, q_v), (resid_in, resid_v), (go_in, go_v), (gr_in, gr_v))
    loads = [
        pltpu.make_async_copy(src, dst, local.at[i]) for i, (src, dst) in enumerate(names)
    ]
    loads.append(pltpu.make_async_copy(k_in, kv.at[c, :, pl.ds(0, kvd)], local.at[5]))
    loads.append(pltpu.make_async_copy(v_in, kv.at[c, :, pl.ds(kvd, kvd)], local.at[6]))
    loads.append(pltpu.make_async_copy(wq_in, w_q.at[f], local.at[7]))
    for copy in loads:
        copy.start()
    greet(planes)
    for slot in (1, 2, 3):
        for i, src in enumerate((k_in, v_in)):
            push(
                src,
                kv.at[c, :, pl.ds(i * kvd, kvd)],
                send,
                recv_kv.at[slot, i],
                c ^ slot,
                f,
            )
    loads[0].wait()
    w_o[f] = wo_v[...].T
    order = by_distance(planes)

    def piece(weight, shard, quarter):
        return quarter_of(full[weight].at[shard], weight, quarter)

    for weight in (0, 1):
        for d in order:
            part = piece(0, f, c) if weight == 0 else quarter_of(wq_in, 1, c)
            push(
                part,
                piece(weight, f, c),
                send,
                recv_z.at[weight, d],
                c,
                shard_at(z, core, planes, d),
            )
        push(
            full[0].at[f] if weight == 0 else wq_in,
            full[weight].at[f],
            send,
            recv_p.at[weight, 0, 0],
            c,
            f ^ 1,
        )
    steps = [(weight, d) for weight in (0, 1) for d in order]
    count = len(steps)

    def to_partner(weight, d, shard, slot):
        part = piece(weight, shard, c ^ slot)
        push(part, part, send, recv_p.at[weight, d, slot], c, f ^ 1)

    def first(weight, d):
        shard = shard_at(z, core, planes, planes - d)
        part = piece(weight, shard, c)
        arrive(part, recv_z.at[weight, d])
        push(part, part, send, recv_x.at[weight, d], c ^ 1, f)
        push(part, part, send, recv_y.at[weight, d], c ^ 2, f)
        to_partner(weight, d, shard, 0)

    def second(weight, d):
        shard = shard_at(z, core, planes, planes - d)
        arrive(piece(weight, shard, c ^ 1), recv_x.at[weight, d])
        arrive(piece(weight, shard, c ^ 2), recv_y.at[weight, d])
        bit = jnp.where(core == weight, 1, 2)
        part = piece(weight, shard, c ^ bit)
        push(part, part, send, recv_d.at[weight, d], c ^ (3 - bit), f)
        to_partner(weight, d, shard, 1)
        to_partner(weight, d, shard, 2)

    def third(weight, d):
        shard = shard_at(z, core, planes, planes - d)
        arrive(piece(weight, shard, c ^ 3), recv_d.at[weight, d])
        to_partner(weight, d, shard, 3)

    def whole_plane(weight, d):
        shard = shard_at(z, core, planes, planes - d) ^ 1
        for slot in range(4):
            arrive(piece(weight, shard, c ^ slot), recv_p.at[weight, d, slot])

    def gather_step(i):
        if i < count:
            first(*steps[i])
        if 0 <= i - 1 < count:
            second(*steps[i - 1])
        if 0 <= i - 2 < count:
            third(*steps[i - 2])

    ends = [lens[0, 0]]
    for i in range(1, lens.shape[1]):
        ends.append(ends[-1] + lens[0, i])

    def document(places):
        number = jnp.zeros(places.shape, jnp.int32)
        for end in ends:
            number = number + (places >= end).astype(jnp.int32)
        return number

    def bias_of(length, first_place, reach):
        shape = (length, toks)
        columns = lax.broadcasted_iota(jnp.int32, shape, 0) + first_place
        rows = lax.broadcasted_iota(jnp.int32, shape, 1) + c * toks
        allowed = (document(columns) == document(rows)) & (columns <= rows)
        if reach:
            allowed = allowed & (columns > rows - reach) & (columns >= 0)
        part = jnp.where(allowed, 0.0, MASKED).astype(f32)
        return jnp.concatenate([part, part], axis=1)

    bias[...] = bias_of(kv.shape[0] * toks, 0, 0)
    bias_b[...] = bias_of(2 * toks, (c - 1) * toks, BAND)

    def paired(tile):
        return jnp.concatenate([tile[:DH], tile[DH:]], axis=1)

    def unpaired(wide):
        return jnp.concatenate([wide[:, :toks], wide[:, toks:]], axis=0)

    wide = 2 * DH

    def scaled(tile):
        return (tile.astype(f32) * scale).astype(bf)

    loads[1].wait()
    for i in range(pairs):
        qp[i] = scaled(paired(q_v[:, wide * i : wide * (i + 1)].T))
    for copy in loads[5:7]:
        copy.wait()
    for slot in (1, 2, 3):
        for i in range(2):
            arrive(kv.at[c ^ slot, :, pl.ds(i * kvd, kvd)], recv_kv.at[slot, i])

    def spread(source, keys_to, values_to, both_t):
        both = source[...].reshape(-1, 2 * kvd)
        for g in range(groups):
            keys_to[g] = both[:, DH * g : DH * (g + 1)]
            values_to[g] = both[:, kvd + DH * g : kvd + DH * (g + 1)]
        turned = both.T
        for g in range(2 * groups):
            both_t[g] = turned[DH * g : DH * (g + 1)]

    spread(kv, kh, vh, kv_t)

    def softmax(scores):
        top = jnp.max(scores, axis=0, keepdims=True)
        raised = jnp.exp(scores - top)
        total = jnp.sum(raised, axis=0, keepdims=True)
        return raised * (1.0 / total)

    def forward(g):
        for j in range(per_group):
            i = per_group * g + j
            weights = softmax(dot(kh[g], qp[i]) + bias[...]).astype(bf)
            probs[i] = weights
            output = dot(kv_t[groups + g], weights).astype(bf)
            o_p[i] = output
            att_t[i // per_shard, i % per_shard] = unpaired(output)

    for g in range(groups):
        forward(g)
        gather_step(g)
    for slot in (1, 2, 3):
        peer = c ^ slot
        push(
            att_t.at[:, peer // 2, pl.ds(pl.multiple_of(lax.rem(peer, 2) * DH, DH), DH), :],
            attq.at[c],
            send,
            recv_att.at[slot],
            peer,
            f,
        )
    attq[c] = att_t[:, c // 2, pl.ds(pl.multiple_of(lax.rem(c, 2) * DH, DH), DH), :]
    for s in range(shards):
        for j in range(per_shard):
            att8[s, :, wide * j : wide * (j + 1)] = att_t[s, j].T
    loads[2].wait()
    loads[3].wait()
    loads[4].wait()
    acc[...] = resid_v[...].astype(f32).T
    for i in range(pairs):
        gp[i] = paired(go_v[:, wide * i : wide * (i + 1)].T)

    def project(weight, shard):
        left = (att8, xb)[weight]
        return dot(left[shard], full[weight][shard]) + dot(left[shard ^ 1], full[weight][shard ^ 1])

    arrive(w_o.at[f ^ 1], recv_p.at[0, 0, 0])
    acc[...] += project(0, f)
    at = groups
    for d in order:
        gather_step(at)
        at += 1
        whole_plane(0, d)
        acc[...] += project(0, shard_at(z, core, planes, planes - d))
    resid = acc[...].astype(bf).astype(f32)
    inverse = lax.rsqrt(jnp.mean(resid * resid, axis=1, keepdims=True) + EPSILON)
    inv[...] = inverse
    values = resid * inverse
    normed[...] = values
    rows_q = w_q.shape[1]
    for s in range(shards):
        xb[s] = values[:, rows_q * s : rows_q * (s + 1)].astype(bf)
    loads[7].wait()
    arrive(w_q.at[f ^ 1], recv_p.at[1, 0, 0])
    acc_p[...] = project(1, f)
    for s in range(shards):
        nt[c, s] = xb[s].T
    for slot in (1, 2, 3):
        push(nt.at[c], nt.at[c], send, recv_nt.at[slot], c ^ slot, f)
    for d in order:
        if at < count + 2:
            gather_step(at)
            at += 1
        whole_plane(1, d)
        acc_p[...] += project(1, shard_at(z, core, planes, planes - d))

    width = qb.shape[0] * wide
    kvx[1] = acc_p[:, width:].astype(bf)
    ahead, behind = (lax.rem(c + 1, 4), lax.rem(c + 3, 4))
    push(kvx.at[1], kvx.at[0], send, recv_halo.at[0], ahead, f)
    for i in range(pairs):
        qb[i] = scaled(paired(acc_p[:, wide * i : wide * (i + 1)].astype(bf).T))
    arrive(kvx.at[0], recv_halo.at[0])
    spread(kvx, khb, vhb, kvx_t)

    def banded(g, carry):
        dk = jnp.zeros((DH, 2 * toks), f32)
        dv = jnp.zeros((DH, 2 * toks), f32)
        for j in range(per_group):
            i = per_group * g + j
            weights = softmax(dot(khb[g], qb[i]) + bias_b[...])
            weights_bf = weights.astype(bf)
            output = dot(kvx_t[groups + g], weights_bf).astype(bf)
            ob_t[i] = unpaired(output)
            grad = gp[i]
            correction = jnp.sum(grad.astype(f32) * output.astype(f32), axis=0, keepdims=True)
            grad_scores = (weights * (dot(vhb[g], grad) - correction)).astype(bf)
            dqb_t[i] = unpaired((dot(kvx_t[g], grad_scores) * scale).astype(bf))
            dk += dot_nt(qb[i], grad_scores)
            dv += dot_nt(grad, weights_bf)
        dkv_b[g] = dk
        dkv_b[groups + g] = dv
        return carry

    lax.fori_loop(0, groups, banded, 0)
    for g in range(2 * groups):
        tail[DH * g : DH * (g + 1)] = dkv_b[g, :, :toks].astype(bf)
    push(tail, head, send, recv_halo.at[1], behind, f)
    gp_width = gp4.shape[2]

    def put_gp(column, block):
        gp4[column // gp_width, :, column % gp_width : column % gp_width + block.shape[1]] = block

    for i in range(pairs):
        out_b[:, wide * i : wide * (i + 1)] = ob_t[i].T
        put_gp(wide * i, dqb_t[i].T)
    arrive(head, recv_halo.at[1])
    own = jnp.concatenate([dkv_b[g, :, toks:] for g in range(2 * groups)], axis=0)
    own = (own + head[...].astype(f32)).astype(bf)
    for i in range(2 * groups * DH // wide):
        put_gp(width + wide * i, own[wide * i : wide * (i + 1)].T)
    for slot in (1, 2, 3):
        push(gp4.at[c ^ slot], gpq.at[c], send, recv_gp.at[slot], c ^ slot, f)
    gpq[c] = gp4[c]

    for s in range(shards):
        total = dot_nt(gp4[0], w_q[s, :, :gp_width])
        for b in range(1, 4):
            total += dot_nt(gp4[b], w_q[s, :, gp_width * b : gp_width * (b + 1)])
        gn[:, rows_q * s : rows_q * (s + 1)] = total
    middle = jnp.mean(gn[...] * normed[...], axis=1, keepdims=True)
    change = inv[...] * (gn[...] - normed[...] * middle)
    grad_mid = gr_v[...].astype(f32).T + change
    gm[c] = grad_mid.astype(bf)
    for slot in (1, 2, 3):
        push(gm.at[c], gm.at[c], send, recv_gm.at[slot], c ^ slot, f)
    out_gm[...] = gm[c].T

    def sum_parts(weight, produce, sent, from_p, from_z, total):
        for d in order[::-1] + [0]:
            sent[d] = produce(shard_at(z, 1 - core, planes, d)).astype(bf)
            push(sent.at[d], from_p.at[d], send, recv_rp.at[weight, d], c, f ^ 1)
        for d in order[::-1] + [0]:
            mine = produce(shard_at(z, core, planes, d))
            arrive(from_p.at[d], recv_rp.at[weight, d])
            mine = mine + from_p[d].astype(f32)
            if d:
                from_z[planes + d] = mine.astype(bf)
                push(
                    from_z.at[planes + d],
                    from_z.at[d],
                    send,
                    recv_rz.at[weight, d],
                    c,
                    shard_at(z, core, planes, d),
                )
            else:
                total[...] = mine

    def finish(weight, from_z, total, result):
        value = total[...]
        for d in range(1, planes):
            arrive(from_z.at[d], recv_rz.at[weight, d])
            value = value + from_z[d].astype(f32)
        result[c] = value.astype(bf)
        for slot in (3, 1, 2):
            push(result.at[c], result.at[c], send, recv_f.at[weight, slot], c ^ slot, f)

    def produce_q(shard):
        left = jnp.concatenate([nt[b, shard] for b in range(4)], axis=1)
        return dot(left, gpq[...].reshape(-1, gp_width))

    def produce_o(shard):
        left = jnp.concatenate([attq[b, shard] for b in range(4)], axis=1)
        return dot(left, gm[...].reshape(-1, gm.shape[2]))

    for s in range(shards):
        part = dot(w_o[s], out_gm[...]).astype(bf)
        for j in range(per_shard):
            gp[per_shard * s + j] = paired(part[wide * j : wide * (j + 1)])
    for slot in (1, 2, 3):
        arrive(nt.at[c ^ slot], recv_nt.at[slot])
        arrive(gpq.at[c ^ slot], recv_gp.at[slot])
    sum_parts(1, produce_q, s_q, p_q, z_q, t_q)

    def backward(g, carry):
        dk = jnp.zeros((DH, 4 * toks), f32)
        dv = jnp.zeros((DH, 4 * toks), f32)
        for j in range(per_group):
            i = per_group * g + j
            grad, weights = (gp[i], probs[i])
            correction = jnp.sum(grad.astype(f32) * o_p[i].astype(f32), axis=0, keepdims=True)
            change = dot(vh[g], grad) - correction
            grad_scores = (weights.astype(f32) * change).astype(bf)
            dqb_t[i] = unpaired((dot(kv_t[g], grad_scores) * scale).astype(bf))
            dk += dot_nt(qp[i], grad_scores)
            dv += dot_nt(grad, weights)
        dkv_t[g] = dk
        dkv_t[groups + g] = dv
        return carry

    lax.fori_loop(0, groups, backward, 0)
    for b in range(4):
        for g in range(2 * groups):
            kvs[b, DH * g : DH * (g + 1)] = dkv_t[g, :, toks * b : toks * (b + 1)].astype(bf)
    for slot in (1, 2, 3):
        push(kvs.at[c ^ slot], kvr.at[slot], send, recv_kvs.at[slot], c ^ slot, f)
    for slot in (1, 2, 3):
        arrive(attq.at[c ^ slot], recv_att.at[slot])
        arrive(gm.at[c ^ slot], recv_gm.at[slot])
    sum_parts(0, produce_o, s_o, p_o, z_o, t_o)
    for i in range(pairs):
        out_dq[:, wide * i : wide * (i + 1)] = dqb_t[i].T
    finish(1, z_q, t_q, res_q)
    total = kvs[c].astype(f32)
    for slot in (1, 2, 3):
        arrive(kvr.at[slot], recv_kvs.at[slot])
        total += kvr[slot].astype(f32)
    total = total.astype(bf).T
    out_dk[...] = total[:, :kvd]
    out_dv[...] = total[:, kvd:]
    finish(0, z_o, t_o, res_o)
    for weight, result in ((1, res_q), (0, res_o)):
        for slot in (3, 1, 2):
            arrive(result.at[c ^ slot], recv_f.at[weight, slot])
    for copy in started:
        copy.wait_send()


def finish_kernel(b_in, gm_in, dq_in, dk_in, dv_in, o_in, q_in, b, gm, dq, dk, dv, wo, wq):
    for src, dst in ((b_in, b), (gm_in, gm), (dq_in, dq), (dk_in, dk), (dv_in, dv)):
        dst[...] = src[...]
    width = q_in.shape[2]
    for quarter in range(4):
        wq[:, width * quarter : width * (quarter + 1)] = q_in[quarter].astype(jnp.float32)
    whole = o_in[...].reshape(-1, o_in.shape[2]).astype(jnp.float32)
    wo[...] = whole.T


def one_kernel(lengths, query, keys, values, resid, w_out, w_qkv, grad_out, grad_resid):
    shards = lax.axis_size("fsdp")
    planes = shards // 2
    bf, f32 = (jnp.bfloat16, jnp.float32)
    toks, hd = query.shape
    kvd = keys.shape[1]
    dim = resid.shape[1]
    rows_o, rows_q = (w_out.shape[0], w_qkv.shape[0])
    width = w_qkv.shape[1]
    wide = 2 * DH
    pairs = hd // wide
    groups = kvd // DH
    seq = 4 * toks
    shape = jax.ShapeDtypeStruct
    o_part, q_part = ((rows_o // 4, dim), (rows_q, width // 4))
    outs = (
        shape((toks, hd), bf),
        shape((dim, toks), bf),
        shape((toks, hd), bf),
        shape((toks, kvd), bf),
        shape((toks, kvd), bf),
        shape((4,) + o_part, bf),
        shape((4,) + q_part, bf),
    )
    v = pltpu.VMEM
    scratch = [
        v((toks, hd), bf),
        v((dim, toks), bf),
        v((dim, rows_o), bf),
        v((toks, hd), bf),
        v((dim, toks), bf),
        v((shards, rows_o, dim), bf),
        v((shards, rows_q, width), bf),
        v((4, toks, 2 * kvd), bf),
        v((groups, seq, DH), bf),
        v((groups, seq, DH), bf),
        v((2 * groups, DH, seq), bf),
        v((pairs, DH, 2 * toks), bf),
        v((pairs, DH, 2 * toks), bf),
        v((seq, 2 * toks), f32),
        v((2 * toks, 2 * toks), f32),
        v((pairs, seq, 2 * toks), bf),
        v((pairs, DH, 2 * toks), bf),
        v((shards, rows_o // wide, wide, toks), bf),
        v((shards, toks, rows_o), bf),
        v((4, shards, rows_o // 4, toks), bf),
        v((toks, dim), f32),
        v((toks, width), f32),
        v((toks, dim), f32),
        v((toks, 1), f32),
        v((shards, toks, rows_q), bf),
        v((4, shards, rows_q, toks), bf),
        v((2, toks, 2 * kvd), bf),
        v((groups, 2 * toks, DH), bf),
        v((groups, 2 * toks, DH), bf),
        v((2 * groups, DH, 2 * toks), bf),
        v((pairs, DH, 2 * toks), bf),
        v((pairs, wide, toks), bf),
        v((pairs, wide, toks), bf),
        v((2 * groups, DH, 2 * toks), f32),
        v((2 * kvd, toks), bf),
        v((2 * kvd, toks), bf),
        v((4, toks, width // 4), bf),
        v((4, toks, width // 4), bf),
        v((toks, dim), f32),
        v((4, toks, dim), bf),
        v((2 * groups, DH, seq), f32),
        v((4, 2 * kvd, toks), bf),
        v((4, 2 * kvd, toks), bf),
    ]
    for part in (q_part, o_part):
        scratch += [
            v((planes,) + part, bf),
            v((planes,) + part, bf),
            v((2 * planes,) + part, bf),
            v(part, f32),
        ]
    dma = pltpu.SemaphoreType.DMA
    scratch += [
        dma((8,)),
        dma,
        dma((4, 2)),
        dma((2, planes)),
        dma((2, planes)),
        dma((2, planes)),
        dma((2, planes)),
        dma((2, planes, 4)),
        dma((4,)),
        dma((4,)),
        dma((2,)),
        dma((4,)),
        dma((4,)),
        dma((4,)),
        dma((2, planes)),
        dma((2, planes)),
        dma((2, 4)),
    ]
    anywhere = pl.BlockSpec(memory_space=pl.ANY)
    in_vmem = pl.BlockSpec(memory_space=pltpu.VMEM)
    results = pl.pallas_call(
        functools.partial(mega_kernel, planes),
        out_shape=outs,
        in_specs=[pl.BlockSpec(memory_space=pltpu.SMEM)] + [anywhere] * 8,
        out_specs=(in_vmem,) * 7,
        scratch_shapes=scratch,
        compiler_params=pltpu.CompilerParams(
            collective_id=0, has_side_effects=True, vmem_limit_bytes=60 * 2**20
        ),
    )(lengths, query, keys, values, resid.T, w_out.T, w_qkv, grad_out, grad_resid.T)
    final = outs[:5] + (shape((dim, rows_o), f32), shape((rows_q, width), f32))
    b, gm, dq, dk, dv, wo, wq = pl.pallas_call(
        finish_kernel,
        out_shape=final,
        in_specs=[in_vmem] * 7,
        out_specs=(in_vmem,) * 7,
    )(*results)
    return (b[None], gm.T[None], dq[None], dk[None], dv[None], wo.T, wq)


def per_device(query_a, key_a, value_a, resid_in, doc_lengths, w_out, w_qkv, grad_out, grad_resid):
    ctx_count = lax.axis_size("ctx")
    ctx_index = lax.axis_index("ctx")
    local_rows = query_a.shape[1]
    seq_len = local_rows * ctx_count
    band_len = BAND
    first_row = ctx_index * local_rows
    documents = doc_table(doc_lengths[0], seq_len)
    fsdp_count = lax.axis_size("fsdp")
    own_kernels = ctx_count == 4 and fsdp_count % 2 == 0 and w_out.shape[0] % 64 == 0
    if own_kernels and local_rows == BAND and w_out.shape[0] == 4 * DH and fsdp_count == 8:
        return one_kernel(
            doc_lengths,
            query_a[0],
            key_a[0],
            value_a[0],
            resid_in[0],
            w_out,
            w_qkv,
            grad_out[0],
            grad_resid[0],
        )
    if own_kernels:
        w_o3, w_b3, kv = gather_weights(
            w_out, w_qkv, jnp.concatenate([key_a[0], value_a[0]], axis=1)
        )
        w_o = w_o3.reshape(-1, w_out.shape[1])
        w_b = w_b3.reshape(-1, w_qkv.shape[1])
        keys, values = (kv[:, : KV * DH], kv[:, KV * DH :])
    else:
        w_o, w_b = (
            lax.all_gather(w_out, "fsdp", axis=0, tiled=True),
            lax.all_gather(w_qkv, "fsdp", axis=0, tiled=True),
        )
        keys, values = (
            lax.all_gather(key_a[0], "ctx", axis=0, tiled=True),
            lax.all_gather(value_a[0], "ctx", axis=0, tiled=True),
        )
    query_t = query_a[0].T
    row_docs = lax.dynamic_slice_in_dim(documents, first_row, local_rows)[None, :]
    row_places = (first_row + jnp.arange(local_rows, dtype=jnp.int32))[None, :]
    columns = jnp.arange(seq_len, dtype=jnp.int32)[:, None]
    allowed_t = ((documents[:, None] == row_docs) & (columns <= row_places)).astype(jnp.float32)
    (attended_t,) = attend(allowed_t, query_t, keys, values)
    attended = attended_t.T
    resid_mid = (
        resid_in[0].astype(jnp.float32) + jnp.dot(attended, w_o, preferred_element_type=jnp.float32)
    ).astype(jnp.bfloat16)
    resid_f = resid_mid.astype(jnp.float32)
    inverse_rms = lax.rsqrt(jnp.mean(resid_f * resid_f, axis=-1, keepdims=True) + EPSILON)
    normed = resid_f * inverse_rms
    normed_bf = normed.astype(jnp.bfloat16)
    projected = jnp.dot(normed_bf, w_b, preferred_element_type=jnp.float32).astype(jnp.bfloat16)
    query_b = projected[:, : H * DH]
    key_b = projected[:, H * DH : H * DH + KV * DH]
    value_b = projected[:, H * DH + KV * DH :]
    tails = from_behind(projected[:, H * DH :], "ctx", 1)
    tail_keys, tail_values = (tails[:, : KV * DH], tails[:, KV * DH :])
    keys_ext = jnp.concatenate([tail_keys, key_b], axis=0)
    values_ext = jnp.concatenate([tail_values, value_b], axis=0)
    doc_pad = jnp.concatenate([jnp.full((band_len,), -1, jnp.int32), documents])
    doc_ext = lax.dynamic_slice_in_dim(doc_pad, first_row, band_len + local_rows)
    ext_places = first_row - band_len + jnp.arange(band_len + local_rows, dtype=jnp.int32)
    ext_places = ext_places[:, None]
    band_t = (doc_ext[:, None] == row_docs) & (ext_places <= row_places)
    band_t = (band_t & (ext_places > row_places - band_len)).astype(jnp.float32)
    banded_t, grad_qb_t, key_heads, value_heads = attend(
        band_t, query_b.T, keys_ext, values_ext, None, grad_out[0].T
    )
    banded, grad_qb = (banded_t.T, grad_qb_t.T)
    key_ext_grad, value_ext_grad = (from_heads(key_heads), from_heads(value_heads))
    heads = jnp.concatenate([key_ext_grad[:band_len], value_ext_grad[:band_len]], axis=1)
    heads = from_behind(heads.astype(jnp.bfloat16), "ctx", -1).astype(jnp.float32)
    head_keys, head_values = (heads[:, : KV * DH], heads[:, KV * DH :])
    grad_kb = key_ext_grad[band_len:].at[local_rows - band_len :].add(head_keys)
    grad_vb = value_ext_grad[band_len:].at[local_rows - band_len :].add(head_values)
    grad_kb = (grad_kb * DH ** (-0.5)).astype(jnp.bfloat16)
    grad_vb = grad_vb.astype(jnp.bfloat16)
    grad_proj = jnp.concatenate([grad_qb, grad_kb, grad_vb], axis=1)
    grad_normed = jnp.dot(grad_proj, w_b.T, preferred_element_type=jnp.float32)
    middle = jnp.mean(grad_normed * normed, axis=-1, keepdims=True)
    grad_mid = (
        grad_resid[0].astype(jnp.float32) + inverse_rms * (grad_normed - normed * middle)
    ).astype(jnp.bfloat16)
    grad_attended = jnp.dot(grad_mid, w_o.T, preferred_element_type=jnp.float32).astype(
        jnp.bfloat16
    )
    grad_query_t, key_heads, value_heads = attend(
        allowed_t, query_t, keys, values, attended_t, grad_attended.T
    )
    grad_query = grad_query_t.T
    key_sums, value_sums = (from_heads(key_heads), from_heads(value_heads))
    if own_kernels:
        norm_t = normed_bf.T.reshape(fsdp_count, -1, local_rows)
        kv_sums = jnp.concatenate([key_sums, value_sums], axis=1).astype(jnp.bfloat16)
        out_share, qkv_share, own_kv = reduce_weights(
            attended_t, norm_t, grad_mid, grad_proj, kv_sums
        )
        own_keys, own_values = (own_kv[:, : KV * DH], own_kv[:, KV * DH :])
        grad_w_out, grad_w_qkv = (out_share.astype(jnp.float32), qkv_share.astype(jnp.float32))
    else:
        own_keys, own_values = (
            lax.psum_scatter(
                key_sums.astype(jnp.bfloat16), "ctx", scatter_dimension=0, tiled=True
            ).astype(jnp.float32),
            lax.psum_scatter(
                value_sums.astype(jnp.bfloat16), "ctx", scatter_dimension=0, tiled=True
            ).astype(jnp.float32),
        )
        piece = normed_bf
        qkv_share = lax.psum_scatter(
            jnp.einsum("tf,tc->fc", piece, grad_proj, preferred_element_type=jnp.float32).astype(
                jnp.bfloat16
            ),
            "fsdp",
            scatter_dimension=0,
            tiled=True,
        )
        piece = attended
        out_share = lax.psum_scatter(
            jnp.einsum("tf,tc->fc", piece, grad_mid, preferred_element_type=jnp.float32).astype(
                jnp.bfloat16
            ),
            "fsdp",
            scatter_dimension=0,
            tiled=True,
        )
        grad_w_out, grad_w_qkv = (
            lax.psum(out_share, "ctx").astype(jnp.float32),
            lax.psum(qkv_share, "ctx").astype(jnp.float32),
        )
    grad_key = (own_keys * DH ** (-0.5)).astype(jnp.bfloat16)
    grad_value = own_values.astype(jnp.bfloat16)
    return (
        banded[None],
        grad_mid[None],
        grad_query[None],
        grad_key[None],
        grad_value[None],
        grad_w_out,
        grad_w_qkv,
    )


def solution(mesh):
    in_specs = (
        P("fsdp", "ctx", None),
        P("fsdp", "ctx", None),
        P("fsdp", "ctx", None),
        P("fsdp", "ctx", None),
        P("fsdp", None),
        P("fsdp", None),
        P("fsdp", None),
        P("fsdp", "ctx", None),
        P("fsdp", "ctx", None),
    )
    out_specs = (
        P("fsdp", "ctx", None),
        P("fsdp", "ctx", None),
        P("fsdp", "ctx", None),
        P("fsdp", "ctx", None),
        P("fsdp", "ctx", None),
        P("fsdp", None),
        P("fsdp", None),
    )
    return jax.shard_map(
        per_device, mesh=mesh, in_specs=in_specs, out_specs=out_specs, check_vma=False
    )
```

```python
import functools

import jax
import jax.numpy as jnp
from jax import lax
from jax.experimental import pallas as pl
from jax.experimental.pallas import tpu as pltpu
from jax.sharding import PartitionSpec as P

H = 32
KV = 4
DH = 64
BAND = 128


MASKED = -1e30
EPSILON = 1e-05


def from_behind(value, axis, steps):
    count = lax.axis_size(axis)
    leading, last = (max(0, -steps), min(count, count - steps))
    return lax.ppermute(value, axis, [(source, source + steps) for source in range(leading, last)])


def doc_table(lengths, seq_len):
    ends = jnp.cumsum(lengths)
    places = jnp.arange(seq_len, dtype=jnp.int32)
    before = places[:, None] >= ends[None, :]
    return jnp.sum(before.astype(jnp.int32), axis=1)


def attend_kernel(with_output, with_grads, *refs):
    refs = list(refs)
    allowed_ref, q_ref, k_ref, v_ref, v_t_ref = refs[:5]
    del refs[:5]
    if with_grads:
        k_t_ref, g_ref = refs[:2]
        del refs[:2]
    o_ref = refs.pop(0)
    if with_grads:
        dq_ref, dk_ref, dv_ref = refs
    allowed = allowed_ref[...] > 0.0
    keys, values, values_t = (k_ref[0], v_ref[0], v_t_ref[...])
    dk = jnp.zeros(keys.shape, jnp.float32)
    dv = jnp.zeros(keys.shape, jnp.float32)
    by_last = (((1,), (1,)), ((), ()))
    for head in range(H // KV):
        rows = slice(head * DH, (head + 1) * DH)
        query = q_ref[rows, :]
        scores = jnp.dot(keys, query, preferred_element_type=jnp.float32) * DH ** (-0.5)
        scores = jnp.where(allowed, scores, MASKED)
        row_max = jnp.max(scores, axis=0, keepdims=True)
        log_total = row_max + jnp.log(
            jnp.sum(jnp.exp(scores - row_max), axis=0, keepdims=True)
        )
        weights = jnp.where(allowed, jnp.exp(scores - log_total), 0.0)
        weights_bf = weights.astype(jnp.bfloat16)
        if with_output:
            output = jnp.dot(values_t, weights_bf, preferred_element_type=jnp.float32)
            output = output.astype(jnp.bfloat16)
            o_ref[rows, :] = output
        else:
            output = o_ref[rows, :]
        if with_grads:
            grad = g_ref[rows, :]
            correction = jnp.sum(
                grad.astype(jnp.float32) * output.astype(jnp.float32), axis=0, keepdims=True
            )
            grad_weights = jnp.dot(values, grad, preferred_element_type=jnp.float32)
            grad_scores = (weights * (grad_weights - correction)).astype(jnp.bfloat16)
            grad_q = jnp.dot(k_t_ref[...], grad_scores, preferred_element_type=jnp.float32)
            dq_ref[rows, :] = (grad_q * DH ** (-0.5)).astype(jnp.bfloat16)
            dk += lax.dot_general(grad_scores, query, by_last, preferred_element_type=jnp.float32)
            dv += lax.dot_general(weights_bf, grad, by_last, preferred_element_type=jnp.float32)
    if with_grads:
        dk_ref[0] = dk
        dv_ref[0] = dv


def by_head(rows):
    return rows.reshape(rows.shape[0], KV, DH).transpose(1, 0, 2)


def from_heads(heads):
    return heads.transpose(1, 0, 2).reshape(heads.shape[1], KV * DH)


def attend(allowed_t, query_t, keys, values, output_t=None, grad_t=None):
    columns, rows = allowed_t.shape
    with_output, with_grads = (output_t is None, grad_t is not None)
    group = pl.BlockSpec((query_t.shape[0] // KV, rows), lambda g: (g, 0))
    key_rows = pl.BlockSpec((1, columns, DH), lambda g: (g, 0, 0))
    key_columns = pl.BlockSpec((DH, columns), lambda g: (g, 0))
    args = [allowed_t, query_t, by_head(keys), by_head(values), values.T]
    in_specs = [pl.BlockSpec((columns, rows), lambda g: (0, 0)), group]
    in_specs += [key_rows, key_rows, key_columns]
    out_shape, out_specs = ([], [])
    wide = jax.ShapeDtypeStruct(query_t.shape, jnp.bfloat16)
    narrow = jax.ShapeDtypeStruct((KV, columns, DH), jnp.float32)
    if with_grads:
        args += [keys.T, grad_t]
        in_specs += [key_columns, group]
    if with_output:
        out_shape.append(wide)
        out_specs.append(group)
    else:
        args.append(output_t)
        in_specs.append(group)
    if with_grads:
        out_shape += [wide, narrow, narrow]
        out_specs += [group, key_rows, key_rows]
    return pl.pallas_call(
        functools.partial(attend_kernel, with_output, with_grads),
        grid=(KV,),
        out_shape=tuple(out_shape),
        in_specs=in_specs,
        out_specs=tuple(out_specs),
    )(*args)


MESH = pl.DeviceIdType.MESH


def remote(src, dst, send_sem, recv_sem, ctx, fsdp):
    return pltpu.make_async_remote_copy(
        src_ref=src,
        dst_ref=dst,
        send_sem=send_sem,
        recv_sem=recv_sem,
        device_id={"ctx": ctx, "fsdp": fsdp},
        device_id_type=MESH,
    )


def place():
    return (lax.axis_index("ctx"), lax.axis_index("fsdp"))


def shard_at(z, core, planes, offset):
    return 2 * lax.rem(z + offset, planes) + core


def greet(planes):
    c, f = place()
    z, core = (f // 2, lax.rem(f, 2))
    barrier = pltpu.get_barrier_semaphore()
    peers = [(c ^ 1, f), (c ^ 2, f), (c ^ 3, f), (c, f ^ 1)]
    peers += [(c, shard_at(z, core, planes, d)) for d in range(1, planes)]
    for ctx, fsdp in peers:
        pl.semaphore_signal(
            barrier, inc=1, device_id={"ctx": ctx, "fsdp": fsdp}, device_id_type=MESH
        )
    pl.semaphore_wait(barrier, len(peers))


def quarter_of(ref, weight, quarter):
    if weight == 0:
        size = ref.shape[0] // 4
        return ref.at[pl.ds(pl.multiple_of(quarter * size, 16), size), :]
    size = ref.shape[1] // 4
    return ref.at[:, pl.ds(pl.multiple_of(quarter * size, 128), size)]


def by_distance(planes):
    order = []
    for step in range(1, planes // 2 + 1):
        for d in (step, planes - step):
            if d not in order:
                order.append(d)
    return order


def gather_kernel(
    planes, wo, wq, kv, go, gq, gkv, send, recv_z, recv_x, recv_y, recv_d, recv_p, recv_kv, local
):
    c, f = place()
    z, core = (f // 2, lax.rem(f, 2))
    mine, full = ((wo, wq), (go, gq))
    rows = kv.shape[0]
    owns = [
        pltpu.make_async_copy(kv, gkv.at[pl.ds(pl.multiple_of(c * rows, 128), rows)], local),
        pltpu.make_async_copy(wo, go.at[f], local),
        pltpu.make_async_copy(wq, gq.at[f], local),
    ]
    for copy in owns:
        copy.start()
    greet(planes)
    started = []

    def push(*args):
        copy = remote(*args)
        copy.start()
        started.append(copy)

    def piece(weight, shard, quarter):
        return quarter_of(full[weight].at[shard], weight, quarter)

    def arrive(ref, sem):
        remote(ref, ref, send, sem, c ^ 1, f).wait_recv()

    kv_place = gkv.at[pl.ds(pl.multiple_of(c * rows, 128), rows)]
    for i, bit in enumerate((1, 2, 3)):
        push(kv, kv_place, send, recv_kv.at[i], c ^ bit, f)
    order = by_distance(planes)
    for weight in (0, 1):
        for d in order:
            push(
                quarter_of(mine[weight], weight, c),
                piece(weight, f, c),
                send,
                recv_z.at[weight, d],
                c,
                shard_at(z, core, planes, d),
            )
        push(mine[weight], full[weight].at[f], send, recv_p.at[weight, 0, 0], c, f ^ 1)
    steps = [(weight, d) for weight in (0, 1) for d in order]

    def to_partner(weight, d, shard, slot):
        part = piece(weight, shard, c ^ slot)
        push(part, part, send, recv_p.at[weight, d, slot], c, f ^ 1)

    def first(weight, d):
        shard = shard_at(z, core, planes, planes - d)
        part = piece(weight, shard, c)
        arrive(part, recv_z.at[weight, d])
        push(part, part, send, recv_x.at[weight, d], c ^ 1, f)
        push(part, part, send, recv_y.at[weight, d], c ^ 2, f)
        to_partner(weight, d, shard, 0)

    def second(weight, d):
        shard = shard_at(z, core, planes, planes - d)
        arrive(piece(weight, shard, c ^ 1), recv_x.at[weight, d])
        arrive(piece(weight, shard, c ^ 2), recv_y.at[weight, d])
        bit = jnp.where(core == weight, 1, 2)
        part = piece(weight, shard, c ^ bit)
        push(part, part, send, recv_d.at[weight, d], c ^ (3 - bit), f)
        to_partner(weight, d, shard, 1)
        to_partner(weight, d, shard, 2)

    def third(weight, d):
        shard = shard_at(z, core, planes, planes - d)
        arrive(piece(weight, shard, c ^ 3), recv_d.at[weight, d])
        to_partner(weight, d, shard, 3)

    count = len(steps)
    for i in range(count + 2):
        if i < count:
            first(*steps[i])
        if 0 <= i - 1 < count:
            second(*steps[i - 1])
        if 0 <= i - 2 < count:
            third(*steps[i - 2])
    for weight in (0, 1):
        arrive(full[weight].at[f ^ 1], recv_p.at[weight, 0, 0])
        for d in order:
            shard = shard_at(z, core, planes, planes - d) ^ 1
            for slot in range(4):
                arrive(piece(weight, shard, c ^ slot), recv_p.at[weight, d, slot])
    for i in range(3):
        arrive(kv_place, recv_kv.at[i])
    for copy in started:
        copy.wait_send()
    for copy in owns:
        copy.wait()


def gather_weights(w_out, w_qkv, kv):
    count = lax.axis_size("fsdp")
    planes = count // 2
    dma = pltpu.SemaphoreType.DMA
    anywhere = pl.BlockSpec(memory_space=pl.ANY)
    return pl.pallas_call(
        functools.partial(gather_kernel, planes),
        out_shape=(
            jax.ShapeDtypeStruct((count,) + w_out.shape, w_out.dtype),
            jax.ShapeDtypeStruct((count,) + w_qkv.shape, w_qkv.dtype),
            jax.ShapeDtypeStruct((4 * kv.shape[0], kv.shape[1]), kv.dtype),
        ),
        in_specs=[anywhere] * 3,
        out_specs=(anywhere,) * 3,
        scratch_shapes=[
            dma,
            dma((2, planes)),
            dma((2, planes)),
            dma((2, planes)),
            dma((2, planes)),
            dma((2, planes, 4)),
            dma((3,)),
            dma,
        ],
        compiler_params=pltpu.CompilerParams(collective_id=0, has_side_effects=True),
    )(w_out, w_qkv, kv)


def reduce_kernel(
    planes,
    att_t,
    norm_t,
    grad_mid,
    grad_proj,
    kv_sums,
    out_o,
    out_q,
    out_kv,
    a_o,
    a_q,
    s_o,
    s_q,
    p_o,
    p_q,
    r1_o,
    r1_q,
    r2_o,
    r2_q,
    rz_o,
    rz_q,
    from_kv,
    send,
    recv_p,
    recv_1,
    recv_2,
    recv_z,
    recv_f,
    recv_kv,
):
    c, f = place()
    z, core = (f // 2, lax.rem(f, 2))
    greet(planes)
    own, sent, from_p, from_1, from_2, from_z, result = (
        (a_o, a_q),
        (s_o, s_q),
        (p_o, p_q),
        (r1_o, r1_q),
        (r2_o, r2_q),
        (rz_o, rz_q),
        (out_o, out_q),
    )
    started = []

    def push(*args):
        copy = remote(*args)
        copy.start()
        started.append(copy)

    def arrive(ref, sem):
        remote(ref, ref, send, sem, c ^ 1, f).wait_recv()

    def term(weight, shard):
        if weight == 0:
            size = a_o.shape[1]
            left = att_t[pl.ds(pl.multiple_of(shard * size, size), size), :]
            right = grad_mid[...]
        else:
            left = norm_t[shard]
            right = grad_proj[...]
        return jnp.dot(left, right, preferred_element_type=jnp.float32).astype(jnp.bfloat16)

    def added(first, second):
        return (first.astype(jnp.float32) + second.astype(jnp.float32)).astype(jnp.bfloat16)

    rows = out_kv.shape[0]

    def kv_rows(index):
        return kv_sums.at[pl.ds(pl.multiple_of(index * rows, rows), rows), :]

    for slot in (3, 1, 2):
        push(
            kv_rows(c ^ slot), from_kv.at[slot], send, recv_kv.at[slot], c ^ slot, f
        )
    order = by_distance(planes)[::-1] + [0]
    steps = [(weight, d) for d in order for weight in (1, 0)]

    def bits(weight):
        bit = jnp.where(core == weight, 1, 2)
        return (bit, 3 - bit)

    def produce(weight, d):
        shard = shard_at(z, core, planes, d)
        sent[weight][d] = term(weight, shard ^ 1)
        push(sent[weight].at[d], from_p[weight].at[d], send, recv_p.at[weight, d], c, f ^ 1)
        own[weight][d] = term(weight, shard)

    def chip_sum(weight, d):
        arrive(from_p[weight].at[d], recv_p.at[weight, d])
        own[weight][d] = added(own[weight][d], from_p[weight][d])
        bit, other = bits(weight)
        for slot, quarter in ((1, c ^ 3), (0, c ^ bit)):
            push(
                quarter_of(own[weight].at[d], weight, quarter),
                from_1[weight].at[d, slot],
                send,
                recv_1.at[weight, d, slot],
                c ^ bit,
                f,
            )

    def pair_sum(weight, d):
        bit, other = bits(weight)
        for slot, quarter in ((1, c ^ other), (0, c)):
            arrive(from_1[weight].at[d, slot], recv_1.at[weight, d, slot])
            part = quarter_of(own[weight].at[d], weight, quarter)
            part[...] = added(part[...], from_1[weight][d, slot])
            if slot == 1:
                push(part, from_2[weight].at[d], send, recv_2.at[weight, d], c ^ other, f)

    def plane_sum(weight, d):
        arrive(from_2[weight].at[d], recv_2.at[weight, d])
        part = quarter_of(own[weight].at[d], weight, c)
        part[...] = added(part[...], from_2[weight][d])
        if d:
            push(
                part,
                from_z[weight].at[d],
                send,
                recv_z.at[weight, d],
                c,
                shard_at(z, core, planes, d),
            )

    def finish(weight):
        part = quarter_of(own[weight].at[0], weight, c)
        total = part[...].astype(jnp.float32)
        for d in range(1, planes):
            arrive(from_z[weight].at[d], recv_z.at[weight, d])
            total = total + from_z[weight][d].astype(jnp.float32)
        place_c = quarter_of(result[weight], weight, c)
        place_c[...] = total.astype(jnp.bfloat16)
        for slot in (3, 1, 2):
            push(place_c, place_c, send, recv_f.at[weight, slot], c ^ slot, f)

    stages = (produce, chip_sum, pair_sum, plane_sum)
    lags = (0, 2, 4, 6)
    count = len(steps)
    for i in range(count + lags[-1]):
        for stage, lag in zip(stages, lags):
            if 0 <= i - lag < count:
                stage(*steps[i - lag])
    kv_total = kv_rows(c)[...].astype(jnp.float32)
    for slot in (1, 2, 3):
        arrive(from_kv.at[slot], recv_kv.at[slot])
        kv_total += from_kv[slot].astype(jnp.float32)
    out_kv[...] = kv_total
    for weight in (1, 0):
        finish(weight)
    for weight in (1, 0):
        for slot in (3, 1, 2):
            arrive(quarter_of(result[weight], weight, c ^ slot), recv_f.at[weight, slot])
    for copy in started:
        copy.wait_send()


def reduce_weights(att_t, norm_t, grad_mid, grad_proj, kv_sums):
    count = lax.axis_size("fsdp")
    planes = count // 2
    dma = pltpu.SemaphoreType.DMA
    in_vmem = pl.BlockSpec(memory_space=pltpu.VMEM)
    bf = jnp.bfloat16
    o_shape = (att_t.shape[0] // count, grad_mid.shape[1])
    q_shape = (norm_t.shape[1], grad_proj.shape[1])
    o_part = (o_shape[0] // 4, o_shape[1])
    q_part = (q_shape[0], q_shape[1] // 4)
    scratch = []
    for lead, shapes in (
        ((planes,), (o_shape, q_shape)),
        ((planes,), (o_shape, q_shape)),
        ((planes,), (o_shape, q_shape)),
        ((planes, 2), (o_part, q_part)),
        ((planes,), (o_part, q_part)),
        ((planes,), (o_part, q_part)),
    ):
        scratch += [pltpu.VMEM(lead + shape, bf) for shape in shapes]
    kv_shape = (kv_sums.shape[0] // 4, kv_sums.shape[1])
    scratch.append(pltpu.VMEM((4,) + kv_shape, bf))
    return pl.pallas_call(
        functools.partial(reduce_kernel, planes),
        out_shape=(
            jax.ShapeDtypeStruct(o_shape, bf),
            jax.ShapeDtypeStruct(q_shape, bf),
            jax.ShapeDtypeStruct(kv_shape, jnp.float32),
        ),
        in_specs=[in_vmem] * 5,
        out_specs=(in_vmem,) * 3,
        scratch_shapes=scratch
        + [
            dma,
            dma((2, planes)),
            dma((2, planes, 2)),
            dma((2, planes)),
            dma((2, planes)),
            dma((2, 4)),
            dma((4,)),
        ],
        compiler_params=pltpu.CompilerParams(
            collective_id=1, has_side_effects=True, vmem_limit_bytes=60 * 2**20
        ),
    )(att_t, norm_t, grad_mid, grad_proj, kv_sums)


def mega_kernel(
    planes,
    lens,
    q_in,
    k_in,
    v_in,
    resid_in,
    wo_in,
    wq_in,
    go_in,
    gr_in,
    out_b,
    out_gm,
    out_dq,
    out_dk,
    out_dv,
    res_o,
    res_q,
    q_v,
    resid_v,
    wo_v,
    go_v,
    gr_v,
    w_o,
    w_q,
    kv,
    kh,
    vh,
    kv_t,
    qp,
    gp,
    bias,
    bias_b,
    probs,
    o_p,
    att_t,
    att8,
    attq,
    acc,
    acc_p,
    normed,
    inv,
    xb,
    nt,
    kvx,
    khb,
    vhb,
    kvx_t,
    qb,
    ob_t,
    dqb_t,
    dkv_b,
    tail,
    head,
    gp4,
    gpq,
    gn,
    gm,
    dkv_t,
    kvs,
    kvr,
    s_q,
    p_q,
    o_q,
    z_q,
    t_q,
    s_o,
    p_o,
    o_o,
    z_o,
    t_o,
    local,
    send,
    recv_kv,
    recv_z,
    recv_x,
    recv_y,
    recv_d,
    recv_p,
    recv_att,
    recv_nt,
    recv_halo,
    recv_gp,
    recv_gm,
    recv_kvs,
    recv_rp,
    recv_rz,
    recv_f,
):
    f32, bf = (jnp.float32, jnp.bfloat16)
    c, f = place()
    z, core = (f // 2, lax.rem(f, 2))
    toks = q_in.shape[0]
    kvd = k_in.shape[1]
    shards = 2 * planes
    groups = kh.shape[0]
    pairs = qp.shape[0]
    per_group = pairs // groups
    per_shard = att_t.shape[1]
    scale = DH ** (-0.5)
    full = (w_o, w_q)
    by_last = (((1,), (1,)), ((), ()))
    started = []

    def push(*args, when=None):
        copy = remote(*args)
        if when is None:
            copy.start()
        else:
            pl.when(when)(copy.start)
        started.append((when, copy))

    def by_plane(table):
        return sum(jnp.where(z == i, entry, 0) for i, entry in enumerate(table))

    near = [sorted((s for s in range(planes) if s != i), key=lambda s: abs(s - i)) for i in range(planes)]
    sources = [by_plane(column) for column in zip(*near)]
    targets = sources[::-1]
    last = planes - 1

    def arrive(ref, sem):
        remote(ref, ref, send, sem, c ^ 1, f).wait_recv()

    def dot(a, b):
        return jnp.dot(a, b, preferred_element_type=f32)

    def dot_nt(a, b):
        return lax.dot_general(a, b, by_last, preferred_element_type=f32)

    def share_rows(ref, sems):
        for bit in (1, 2):
            push(ref.at[c], ref.at[c], send, sems.at[bit], c ^ bit, f)

    def relay_rows(ref, sems):
        half = ref.shape[1] // 2
        for bit in (1, 2):
            arrive(ref.at[c ^ bit], sems.at[bit])
            part = ref.at[c ^ bit, pl.ds((bit - 1) * half, half)]
            push(part, part, send, sems.at[2 + bit], c ^ (3 - bit), f)

    def far_rows(ref, sems):
        half = ref.shape[1] // 2
        for bit in (1, 2):
            arrive(ref.at[c ^ 3, pl.ds((bit - 1) * half, half)], sems.at[2 + bit])

    names = ((wo_in, wo_v), (q_in, q_v), (resid_in, resid_v), (go_in, go_v), (gr_in, gr_v))
    loads = [
        pltpu.make_async_copy(src, dst, local.at[i]) for i, (src, dst) in enumerate(names)
    ]
    loads.append(pltpu.make_async_copy(k_in, kv.at[c, :, pl.ds(0, kvd)], local.at[5]))
    loads.append(pltpu.make_async_copy(v_in, kv.at[c, :, pl.ds(kvd, kvd)], local.at[6]))
    loads.append(pltpu.make_async_copy(wq_in, w_q.at[f], local.at[7]))
    for copy in loads:
        copy.start()
    greet(planes)
    for slot in (1, 2, 3):
        for i, src in enumerate((k_in, v_in)):
            push(
                src,
                kv.at[c, :, pl.ds(i * kvd, kvd)],
                send,
                recv_kv.at[slot, i],
                c ^ slot,
                f,
            )
    loads[0].wait()
    w_o[f] = wo_v[...].T
    slots = range(planes - 1)

    def piece(weight, shard, quarter):
        return quarter_of(full[weight].at[shard], weight, quarter)

    def share(weight):
        mine = w_o.at[f] if weight == 0 else wq_in
        for plane, ok in ((z + 1, z < last), (z - 1, z > 0)):
            push(
                quarter_of(mine, weight, c),
                piece(weight, f, c),
                send,
                recv_z.at[weight, z],
                c,
                2 * plane + core,
                when=ok,
            )
        push(mine, full[weight].at[f], send, recv_p.at[weight, 0, 0], c, f ^ 1)

    share(0)
    steps = [(weight, d) for weight in (0, 1) for d in slots]
    count = len(steps)

    def to_partner(weight, d, shard, slot):
        part = piece(weight, shard, c ^ slot)
        push(part, part, send, recv_p.at[weight, d + 1, slot], c, f ^ 1)

    def first(weight, d):
        source = sources[d]
        shard = 2 * source + core
        part = piece(weight, shard, c)
        arrive(part, recv_z.at[weight, source])
        onward = jnp.where(source < z, z < last, z > 0)
        plane = jnp.where(source < z, z + 1, z - 1)
        push(part, part, send, recv_z.at[weight, source], c, 2 * plane + core, when=onward)
        push(part, part, send, recv_x.at[weight, d], c ^ 1, f)
        push(part, part, send, recv_y.at[weight, d], c ^ 2, f)
        to_partner(weight, d, shard, 0)

    def second(weight, d):
        shard = 2 * sources[d] + core
        arrive(piece(weight, shard, c ^ 1), recv_x.at[weight, d])
        arrive(piece(weight, shard, c ^ 2), recv_y.at[weight, d])
        bit = jnp.where(core == weight, 1, 2)
        part = piece(weight, shard, c ^ bit)
        push(part, part, send, recv_d.at[weight, d], c ^ (3 - bit), f)
        to_partner(weight, d, shard, 1)
        to_partner(weight, d, shard, 2)

    def third(weight, d):
        shard = 2 * sources[d] + core
        arrive(piece(weight, shard, c ^ 3), recv_d.at[weight, d])
        to_partner(weight, d, shard, 3)

    def whole_plane(weight, d):
        shard = 2 * sources[d] + 1 - core
        for slot in range(4):
            arrive(piece(weight, shard, c ^ slot), recv_p.at[weight, d + 1, slot])

    def gather_step(i):
        if i < count:
            first(*steps[i])
        if 0 <= i - 1 < count:
            second(*steps[i - 1])
        if 0 <= i - 2 < count:
            third(*steps[i - 2])

    ends = [lens[0, 0]]
    for i in range(1, lens.shape[1]):
        ends.append(ends[-1] + lens[0, i])

    def document(places):
        number = jnp.zeros(places.shape, jnp.int32)
        for end in ends:
            number = number + (places >= end).astype(jnp.int32)
        return number

    def bias_of(length, first_place, reach):
        shape = (length, toks)
        columns = lax.broadcasted_iota(jnp.int32, shape, 0) + first_place
        rows = lax.broadcasted_iota(jnp.int32, shape, 1) + c * toks
        allowed = (document(columns) == document(rows)) & (columns <= rows)
        if reach:
            allowed = allowed & (columns > rows - reach) & (columns >= 0)
        part = jnp.where(allowed, 0.0, MASKED).astype(f32)
        return jnp.concatenate([part, part], axis=1)

    bias[...] = bias_of(kv.shape[0] * toks, 0, 0)
    bias_b[...] = bias_of(2 * toks, (c - 1) * toks, BAND)

    def paired(tile):
        return jnp.concatenate([tile[:DH], tile[DH:]], axis=1)

    def unpaired(wide):
        return jnp.concatenate([wide[:, :toks], wide[:, toks:]], axis=0)

    wide = 2 * DH

    def scaled(tile):
        return (tile.astype(f32) * scale).astype(bf)

    loads[1].wait()
    for i in range(pairs):
        qp[i] = scaled(paired(q_v[:, wide * i : wide * (i + 1)].T))
    for copy in loads[5:7]:
        copy.wait()
    for slot in (1, 2, 3):
        for i in range(2):
            arrive(kv.at[c ^ slot, :, pl.ds(i * kvd, kvd)], recv_kv.at[slot, i])

    def spread(source, keys_to, values_to, both_t):
        both = source[...].reshape(-1, 2 * kvd)
        for g in range(groups):
            keys_to[g] = both[:, DH * g : DH * (g + 1)]
            values_to[g] = both[:, kvd + DH * g : kvd + DH * (g + 1)]
        turned = both.T
        for g in range(2 * groups):
            both_t[g] = turned[DH * g : DH * (g + 1)]

    spread(kv, kh, vh, kv_t)

    def softmax(scores):
        top = jnp.max(scores, axis=0, keepdims=True)
        raised = jnp.exp(scores - top)
        total = jnp.sum(raised, axis=0, keepdims=True)
        return raised * (1.0 / total)

    def forward(g):
        for j in range(per_group):
            i = per_group * g + j
            weights = softmax(dot(kh[g], qp[i]) + bias[...]).astype(bf)
            probs[i] = weights
            output = dot(kv_t[groups + g], weights).astype(bf)
            o_p[i] = output
            att_t[i // per_shard, i % per_shard] = unpaired(output)

    for g in range(groups):
        gather_step(g)
        if g == 1:
            share(1)
        forward(g)
    attq[c] = att_t[:, c // 2, pl.ds(pl.multiple_of(lax.rem(c, 2) * DH, DH), DH), :]
    for s in range(shards):
        for j in range(per_shard):
            att8[s, :, wide * j : wide * (j + 1)] = att_t[s, j].T
    loads[2].wait()
    loads[3].wait()
    loads[4].wait()
    acc[...] = resid_v[...].astype(f32).T
    for i in range(pairs):
        gp[i] = paired(go_v[:, wide * i : wide * (i + 1)].T)

    def project(weight, shard):
        left = (att8, xb)[weight]
        return dot(left[shard], full[weight][shard]) + dot(left[shard ^ 1], full[weight][shard ^ 1])

    arrive(w_o.at[f ^ 1], recv_p.at[0, 0, 0])
    acc[...] += project(0, f)
    at = groups
    for d in slots:
        gather_step(at)
        at += 1
        whole_plane(0, d)
        acc[...] += project(0, 2 * sources[d] + core)
    resid = acc[...].astype(bf).astype(f32)
    inverse = lax.rsqrt(jnp.mean(resid * resid, axis=1, keepdims=True) + EPSILON)
    inv[...] = inverse
    values = resid * inverse
    normed[...] = values
    rows_q = w_q.shape[1]
    for s in range(shards):
        xb[s] = values[:, rows_q * s : rows_q * (s + 1)].astype(bf)
    loads[7].wait()
    arrive(w_q.at[f ^ 1], recv_p.at[1, 0, 0])
    acc_p[...] = project(1, f)
    for s in range(shards):
        nt[c, s] = xb[s].T
    for d in slots:
        if at < count + 2:
            gather_step(at)
            at += 1
        whole_plane(1, d)
        acc_p[...] += project(1, 2 * sources[d] + core)

    width = qb.shape[0] * wide
    kvx[1] = acc_p[:, width:].astype(bf)
    ahead, behind = (lax.rem(c + 1, 4), lax.rem(c + 3, 4))
    push(kvx.at[1], kvx.at[0], send, recv_halo.at[0], ahead, f)
    share_rows(nt, recv_nt)
    for i in range(pairs):
        qb[i] = scaled(paired(acc_p[:, wide * i : wide * (i + 1)].astype(bf).T))
    arrive(kvx.at[0], recv_halo.at[0])
    spread(kvx, khb, vhb, kvx_t)

    def banded(g, carry):
        dk = jnp.zeros((DH, 2 * toks), f32)
        dv = jnp.zeros((DH, 2 * toks), f32)
        for j in range(per_group):
            i = per_group * g + j
            weights = softmax(dot(khb[g], qb[i]) + bias_b[...])
            weights_bf = weights.astype(bf)
            output = dot(kvx_t[groups + g], weights_bf).astype(bf)
            ob_t[i] = unpaired(output)
            grad = gp[i]
            correction = jnp.sum(grad.astype(f32) * output.astype(f32), axis=0, keepdims=True)
            grad_scores = (weights * (dot(vhb[g], grad) - correction)).astype(bf)
            dqb_t[i] = unpaired((dot(kvx_t[g], grad_scores) * scale).astype(bf))
            dk += dot_nt(qb[i], grad_scores)
            dv += dot_nt(grad, weights_bf)
        dkv_b[g] = dk
        dkv_b[groups + g] = dv
        return carry

    lax.fori_loop(0, groups, banded, 0)
    for g in range(2 * groups):
        tail[DH * g : DH * (g + 1)] = dkv_b[g, :, :toks].astype(bf)
    push(tail, head, send, recv_halo.at[1], behind, f)
    relay_rows(nt, recv_nt)
    gp_width = gp4.shape[2]

    def put_gp(column, block):
        gp4[column // gp_width, :, column % gp_width : column % gp_width + block.shape[1]] = block

    for i in range(pairs):
        out_b[:, wide * i : wide * (i + 1)] = ob_t[i].T
        put_gp(wide * i, dqb_t[i].T)
    arrive(head, recv_halo.at[1])
    own = jnp.concatenate([dkv_b[g, :, toks:] for g in range(2 * groups)], axis=0)
    own = (own + head[...].astype(f32)).astype(bf)
    for i in range(2 * groups * DH // wide):
        put_gp(width + wide * i, own[wide * i : wide * (i + 1)].T)
    for slot in (1, 2, 3):
        push(gp4.at[c ^ slot], gpq.at[c], send, recv_gp.at[slot], c ^ slot, f)
    gpq[c] = gp4[c]

    for s in range(shards):
        total = dot_nt(gp4[0], w_q[s, :, :gp_width])
        for b in range(1, 4):
            total += dot_nt(gp4[b], w_q[s, :, gp_width * b : gp_width * (b + 1)])
        gn[:, rows_q * s : rows_q * (s + 1)] = total
    middle = jnp.mean(gn[...] * normed[...], axis=1, keepdims=True)
    change = inv[...] * (gn[...] - normed[...] * middle)
    grad_mid = gr_v[...].astype(f32).T + change
    gm[c] = grad_mid.astype(bf)
    share_rows(gm, recv_gm)
    for slot in (1, 2, 3):
        peer = c ^ slot
        push(
            att_t.at[:, peer // 2, pl.ds(pl.multiple_of(lax.rem(peer, 2) * DH, DH), DH), :],
            attq.at[c],
            send,
            recv_att.at[slot],
            peer,
            f,
        )
    out_gm[...] = gm[c].T

    def sum_chip(weight, produce, sent, from_p, totals):
        for d in range(planes):
            sent[d] = produce(2 * d + 1 - core).astype(bf)
            push(sent.at[d], from_p.at[d], send, recv_rp.at[weight, d], c, f ^ 1)
        for d in range(planes):
            mine = produce(2 * d + core)
            arrive(from_p.at[d], recv_rp.at[weight, d])
            totals[d] = mine + from_p[d].astype(f32)

    def chain(weight, slot, totals, out, moving):
        target = targets[slot]
        way = jnp.where(target > z, 0, 1)
        plane = jnp.where(target > z, z + 1, z - 1)

        @pl.when(jnp.where(target > z, z > 0, z < last))
        def _():
            arrive(moving.at[way, target], recv_rz.at[weight, way, target])
            totals[target] += moving[way, target].astype(f32)

        out[slot] = totals[target].astype(bf)
        push(
            out.at[slot],
            moving.at[way, target],
            send,
            recv_rz.at[weight, way, target],
            c,
            2 * plane + core,
        )

    def finish(weight, totals, moving, result):
        for way, ok in ((0, z > 0), (1, z < last)):

            @pl.when(ok)
            def _():
                arrive(moving.at[way, z], recv_rz.at[weight, way, z])
                totals[z] += moving[way, z].astype(f32)

        result[c] = totals[z].astype(bf)
        for slot in (3, 1, 2):
            push(result.at[c], result.at[c], send, recv_f.at[weight, slot], c ^ slot, f)

    def produce_q(shard):
        left = jnp.concatenate([nt[b, shard] for b in range(4)], axis=1)
        return dot(left, gpq[...].reshape(-1, gp_width))

    def produce_o(shard):
        left = jnp.concatenate([attq[b, shard] for b in range(4)], axis=1)
        return dot(left, gm[...].reshape(-1, gm.shape[2]))

    far_rows(nt, recv_nt)
    for slot in (1, 2, 3):
        arrive(gpq.at[c ^ slot], recv_gp.at[slot])
    sum_chip(1, produce_q, s_q, p_q, t_q)
    chain(1, 0, t_q, o_q, z_q)
    for s in range(shards):
        part = dot(w_o[s], out_gm[...]).astype(bf)
        for j in range(per_shard):
            gp[per_shard * s + j] = paired(part[wide * j : wide * (j + 1)])
    chain(1, 1, t_q, o_q, z_q)
    relay_rows(gm, recv_gm)

    def backward(g, carry):
        dk = jnp.zeros((DH, 4 * toks), f32)
        dv = jnp.zeros((DH, 4 * toks), f32)
        for j in range(per_group):
            i = per_group * g + j
            grad, weights = (gp[i], probs[i])
            correction = jnp.sum(grad.astype(f32) * o_p[i].astype(f32), axis=0, keepdims=True)
            change = dot(vh[g], grad) - correction
            grad_scores = (weights.astype(f32) * change).astype(bf)
            dqb_t[i] = unpaired((dot(kv_t[g], grad_scores) * scale).astype(bf))
            dk += dot_nt(qp[i], grad_scores)
            dv += dot_nt(grad, weights)
        dkv_t[g] = dk
        dkv_t[groups + g] = dv
        return carry

    lax.fori_loop(0, groups // 2, backward, 0)
    for slot in slots[2:]:
        chain(1, slot, t_q, o_q, z_q)
    lax.fori_loop(groups // 2, groups, backward, 0)
    for b in range(4):
        for g in range(2 * groups):
            kvs[b, DH * g : DH * (g + 1)] = dkv_t[g, :, toks * b : toks * (b + 1)].astype(bf)
    for slot in (1, 2, 3):
        push(kvs.at[c ^ slot], kvr.at[slot], send, recv_kvs.at[slot], c ^ slot, f)
    for slot in (1, 2, 3):
        arrive(attq.at[c ^ slot], recv_att.at[slot])
    far_rows(gm, recv_gm)
    sum_chip(0, produce_o, s_o, p_o, t_o)
    chain(0, 0, t_o, o_o, z_o)
    for i in range(pairs):
        out_dq[:, wide * i : wide * (i + 1)] = dqb_t[i].T
    finish(1, t_q, z_q, res_q)
    for slot in slots[1:]:
        chain(0, slot, t_o, o_o, z_o)
    total = kvs[c].astype(f32)
    for slot in (1, 2, 3):
        arrive(kvr.at[slot], recv_kvs.at[slot])
        total += kvr[slot].astype(f32)
    total = total.astype(bf).T
    out_dk[...] = total[:, :kvd]
    out_dv[...] = total[:, kvd:]
    finish(0, t_o, z_o, res_o)
    for weight, result in ((1, res_q), (0, res_o)):
        for slot in (3, 1, 2):
            arrive(result.at[c ^ slot], recv_f.at[weight, slot])
    for when, copy in started:
        if when is None:
            copy.wait_send()
        else:
            pl.when(when)(copy.wait_send)


def finish_kernel(b_in, gm_in, dq_in, dk_in, dv_in, o_in, q_in, b, gm, dq, dk, dv, wo, wq):
    for src, dst in ((b_in, b), (gm_in, gm), (dq_in, dq), (dk_in, dk), (dv_in, dv)):
        dst[...] = src[...]
    width = q_in.shape[2]
    for quarter in range(4):
        wq[:, width * quarter : width * (quarter + 1)] = q_in[quarter].astype(jnp.float32)
    whole = o_in[...].reshape(-1, o_in.shape[2]).astype(jnp.float32)
    wo[...] = whole.T


def one_kernel(lengths, query, keys, values, resid, w_out, w_qkv, grad_out, grad_resid):
    shards = lax.axis_size("fsdp")
    planes = shards // 2
    bf, f32 = (jnp.bfloat16, jnp.float32)
    toks, hd = query.shape
    kvd = keys.shape[1]
    dim = resid.shape[1]
    rows_o, rows_q = (w_out.shape[0], w_qkv.shape[0])
    width = w_qkv.shape[1]
    wide = 2 * DH
    pairs = hd // wide
    groups = kvd // DH
    seq = 4 * toks
    shape = jax.ShapeDtypeStruct
    o_part, q_part = ((rows_o // 4, dim), (rows_q, width // 4))
    outs = (
        shape((toks, hd), bf),
        shape((dim, toks), bf),
        shape((toks, hd), bf),
        shape((toks, kvd), bf),
        shape((toks, kvd), bf),
        shape((4,) + o_part, bf),
        shape((4,) + q_part, bf),
    )
    v = pltpu.VMEM
    scratch = [
        v((toks, hd), bf),
        v((dim, toks), bf),
        v((dim, rows_o), bf),
        v((toks, hd), bf),
        v((dim, toks), bf),
        v((shards, rows_o, dim), bf),
        v((shards, rows_q, width), bf),
        v((4, toks, 2 * kvd), bf),
        v((groups, seq, DH), bf),
        v((groups, seq, DH), bf),
        v((2 * groups, DH, seq), bf),
        v((pairs, DH, 2 * toks), bf),
        v((pairs, DH, 2 * toks), bf),
        v((seq, 2 * toks), f32),
        v((2 * toks, 2 * toks), f32),
        v((pairs, seq, 2 * toks), bf),
        v((pairs, DH, 2 * toks), bf),
        v((shards, rows_o // wide, wide, toks), bf),
        v((shards, toks, rows_o), bf),
        v((4, shards, rows_o // 4, toks), bf),
        v((toks, dim), f32),
        v((toks, width), f32),
        v((toks, dim), f32),
        v((toks, 1), f32),
        v((shards, toks, rows_q), bf),
        v((4, shards, rows_q, toks), bf),
        v((2, toks, 2 * kvd), bf),
        v((groups, 2 * toks, DH), bf),
        v((groups, 2 * toks, DH), bf),
        v((2 * groups, DH, 2 * toks), bf),
        v((pairs, DH, 2 * toks), bf),
        v((pairs, wide, toks), bf),
        v((pairs, wide, toks), bf),
        v((2 * groups, DH, 2 * toks), f32),
        v((2 * kvd, toks), bf),
        v((2 * kvd, toks), bf),
        v((4, toks, width // 4), bf),
        v((4, toks, width // 4), bf),
        v((toks, dim), f32),
        v((4, toks, dim), bf),
        v((2 * groups, DH, seq), f32),
        v((4, 2 * kvd, toks), bf),
        v((4, 2 * kvd, toks), bf),
    ]
    for part in (q_part, o_part):
        scratch += [
            v((planes,) + part, bf),
            v((planes,) + part, bf),
            v((planes,) + part, bf),
            v((2, planes) + part, bf),
            v((planes,) + part, f32),
        ]
    dma = pltpu.SemaphoreType.DMA
    scratch += [
        dma((8,)),
        dma,
        dma((4, 2)),
        dma((2, planes)),
        dma((2, planes)),
        dma((2, planes)),
        dma((2, planes)),
        dma((2, planes, 4)),
        dma((4,)),
        dma((5,)),
        dma((2,)),
        dma((4,)),
        dma((5,)),
        dma((4,)),
        dma((2, planes)),
        dma((2, 2, planes)),
        dma((2, 4)),
    ]
    anywhere = pl.BlockSpec(memory_space=pl.ANY)
    in_vmem = pl.BlockSpec(memory_space=pltpu.VMEM)
    results = pl.pallas_call(
        functools.partial(mega_kernel, planes),
        out_shape=outs,
        in_specs=[pl.BlockSpec(memory_space=pltpu.SMEM)] + [anywhere] * 8,
        out_specs=(in_vmem,) * 7,
        scratch_shapes=scratch,
        compiler_params=pltpu.CompilerParams(
            collective_id=0, has_side_effects=True, vmem_limit_bytes=60 * 2**20
        ),
    )(lengths, query, keys, values, resid.T, w_out.T, w_qkv, grad_out, grad_resid.T)
    final = outs[:5] + (shape((dim, rows_o), f32), shape((rows_q, width), f32))
    b, gm, dq, dk, dv, wo, wq = pl.pallas_call(
        finish_kernel,
        out_shape=final,
        in_specs=[in_vmem] * 7,
        out_specs=(in_vmem,) * 7,
    )(*results)
    return (b[None], gm.T[None], dq[None], dk[None], dv[None], wo.T, wq)


def per_device(query_a, key_a, value_a, resid_in, doc_lengths, w_out, w_qkv, grad_out, grad_resid):
    ctx_count = lax.axis_size("ctx")
    ctx_index = lax.axis_index("ctx")
    local_rows = query_a.shape[1]
    seq_len = local_rows * ctx_count
    band_len = BAND
    first_row = ctx_index * local_rows
    documents = doc_table(doc_lengths[0], seq_len)
    fsdp_count = lax.axis_size("fsdp")
    own_kernels = ctx_count == 4 and fsdp_count % 2 == 0 and w_out.shape[0] % 64 == 0
    if own_kernels and local_rows == BAND and w_out.shape[0] == 4 * DH and fsdp_count == 8:
        return one_kernel(
            doc_lengths,
            query_a[0],
            key_a[0],
            value_a[0],
            resid_in[0],
            w_out,
            w_qkv,
            grad_out[0],
            grad_resid[0],
        )
    if own_kernels:
        w_o3, w_b3, kv = gather_weights(
            w_out, w_qkv, jnp.concatenate([key_a[0], value_a[0]], axis=1)
        )
        w_o = w_o3.reshape(-1, w_out.shape[1])
        w_b = w_b3.reshape(-1, w_qkv.shape[1])
        keys, values = (kv[:, : KV * DH], kv[:, KV * DH :])
    else:
        w_o, w_b = (
            lax.all_gather(w_out, "fsdp", axis=0, tiled=True),
            lax.all_gather(w_qkv, "fsdp", axis=0, tiled=True),
        )
        keys, values = (
            lax.all_gather(key_a[0], "ctx", axis=0, tiled=True),
            lax.all_gather(value_a[0], "ctx", axis=0, tiled=True),
        )
    query_t = query_a[0].T
    row_docs = lax.dynamic_slice_in_dim(documents, first_row, local_rows)[None, :]
    row_places = (first_row + jnp.arange(local_rows, dtype=jnp.int32))[None, :]
    columns = jnp.arange(seq_len, dtype=jnp.int32)[:, None]
    allowed_t = ((documents[:, None] == row_docs) & (columns <= row_places)).astype(jnp.float32)
    (attended_t,) = attend(allowed_t, query_t, keys, values)
    attended = attended_t.T
    resid_mid = (
        resid_in[0].astype(jnp.float32) + jnp.dot(attended, w_o, preferred_element_type=jnp.float32)
    ).astype(jnp.bfloat16)
    resid_f = resid_mid.astype(jnp.float32)
    inverse_rms = lax.rsqrt(jnp.mean(resid_f * resid_f, axis=-1, keepdims=True) + EPSILON)
    normed = resid_f * inverse_rms
    normed_bf = normed.astype(jnp.bfloat16)
    projected = jnp.dot(normed_bf, w_b, preferred_element_type=jnp.float32).astype(jnp.bfloat16)
    query_b = projected[:, : H * DH]
    key_b = projected[:, H * DH : H * DH + KV * DH]
    value_b = projected[:, H * DH + KV * DH :]
    tails = from_behind(projected[:, H * DH :], "ctx", 1)
    tail_keys, tail_values = (tails[:, : KV * DH], tails[:, KV * DH :])
    keys_ext = jnp.concatenate([tail_keys, key_b], axis=0)
    values_ext = jnp.concatenate([tail_values, value_b], axis=0)
    doc_pad = jnp.concatenate([jnp.full((band_len,), -1, jnp.int32), documents])
    doc_ext = lax.dynamic_slice_in_dim(doc_pad, first_row, band_len + local_rows)
    ext_places = first_row - band_len + jnp.arange(band_len + local_rows, dtype=jnp.int32)
    ext_places = ext_places[:, None]
    band_t = (doc_ext[:, None] == row_docs) & (ext_places <= row_places)
    band_t = (band_t & (ext_places > row_places - band_len)).astype(jnp.float32)
    banded_t, grad_qb_t, key_heads, value_heads = attend(
        band_t, query_b.T, keys_ext, values_ext, None, grad_out[0].T
    )
    banded, grad_qb = (banded_t.T, grad_qb_t.T)
    key_ext_grad, value_ext_grad = (from_heads(key_heads), from_heads(value_heads))
    heads = jnp.concatenate([key_ext_grad[:band_len], value_ext_grad[:band_len]], axis=1)
    heads = from_behind(heads.astype(jnp.bfloat16), "ctx", -1).astype(jnp.float32)
    head_keys, head_values = (heads[:, : KV * DH], heads[:, KV * DH :])
    grad_kb = key_ext_grad[band_len:].at[local_rows - band_len :].add(head_keys)
    grad_vb = value_ext_grad[band_len:].at[local_rows - band_len :].add(head_values)
    grad_kb = (grad_kb * DH ** (-0.5)).astype(jnp.bfloat16)
    grad_vb = grad_vb.astype(jnp.bfloat16)
    grad_proj = jnp.concatenate([grad_qb, grad_kb, grad_vb], axis=1)
    grad_normed = jnp.dot(grad_proj, w_b.T, preferred_element_type=jnp.float32)
    middle = jnp.mean(grad_normed * normed, axis=-1, keepdims=True)
    grad_mid = (
        grad_resid[0].astype(jnp.float32) + inverse_rms * (grad_normed - normed * middle)
    ).astype(jnp.bfloat16)
    grad_attended = jnp.dot(grad_mid, w_o.T, preferred_element_type=jnp.float32).astype(
        jnp.bfloat16
    )
    grad_query_t, key_heads, value_heads = attend(
        allowed_t, query_t, keys, values, attended_t, grad_attended.T
    )
    grad_query = grad_query_t.T
    key_sums, value_sums = (from_heads(key_heads), from_heads(value_heads))
    if own_kernels:
        norm_t = normed_bf.T.reshape(fsdp_count, -1, local_rows)
        kv_sums = jnp.concatenate([key_sums, value_sums], axis=1).astype(jnp.bfloat16)
        out_share, qkv_share, own_kv = reduce_weights(
            attended_t, norm_t, grad_mid, grad_proj, kv_sums
        )
        own_keys, own_values = (own_kv[:, : KV * DH], own_kv[:, KV * DH :])
        grad_w_out, grad_w_qkv = (out_share.astype(jnp.float32), qkv_share.astype(jnp.float32))
    else:
        own_keys, own_values = (
            lax.psum_scatter(
                key_sums.astype(jnp.bfloat16), "ctx", scatter_dimension=0, tiled=True
            ).astype(jnp.float32),
            lax.psum_scatter(
                value_sums.astype(jnp.bfloat16), "ctx", scatter_dimension=0, tiled=True
            ).astype(jnp.float32),
        )
        piece = normed_bf
        qkv_share = lax.psum_scatter(
            jnp.einsum("tf,tc->fc", piece, grad_proj, preferred_element_type=jnp.float32).astype(
                jnp.bfloat16
            ),
            "fsdp",
            scatter_dimension=0,
            tiled=True,
        )
        piece = attended
        out_share = lax.psum_scatter(
            jnp.einsum("tf,tc->fc", piece, grad_mid, preferred_element_type=jnp.float32).astype(
                jnp.bfloat16
            ),
            "fsdp",
            scatter_dimension=0,
            tiled=True,
        )
        grad_w_out, grad_w_qkv = (
            lax.psum(out_share, "ctx").astype(jnp.float32),
            lax.psum(qkv_share, "ctx").astype(jnp.float32),
        )
    grad_key = (own_keys * DH ** (-0.5)).astype(jnp.bfloat16)
    grad_value = own_values.astype(jnp.bfloat16)
    return (
        banded[None],
        grad_mid[None],
        grad_query[None],
        grad_key[None],
        grad_value[None],
        grad_w_out,
        grad_w_qkv,
    )


def solution(mesh):
    in_specs = (
        P("fsdp", "ctx", None),
        P("fsdp", "ctx", None),
        P("fsdp", "ctx", None),
        P("fsdp", "ctx", None),
        P("fsdp", None),
        P("fsdp", None),
        P("fsdp", None),
        P("fsdp", "ctx", None),
        P("fsdp", "ctx", None),
    )
    out_specs = (
        P("fsdp", "ctx", None),
        P("fsdp", "ctx", None),
        P("fsdp", "ctx", None),
        P("fsdp", "ctx", None),
        P("fsdp", "ctx", None),
        P("fsdp", None),
        P("fsdp", None),
    )
    return jax.shard_map(
        per_device, mesh=mesh, in_specs=in_specs, out_specs=out_specs, check_vma=False
    )
```

```python
import functools

import jax
import jax.numpy as jnp
from jax import lax
from jax.experimental import pallas as pl
from jax.experimental.pallas import tpu as pltpu
from jax.sharding import PartitionSpec as P

H = 32
KV = 4
DH = 64
BAND = 128


MASKED = -1e30
EPSILON = 1e-05


def from_behind(value, axis, steps):
    count = lax.axis_size(axis)
    leading, last = (max(0, -steps), min(count, count - steps))
    return lax.ppermute(value, axis, [(source, source + steps) for source in range(leading, last)])


def doc_table(lengths, seq_len):
    ends = jnp.cumsum(lengths)
    places = jnp.arange(seq_len, dtype=jnp.int32)
    before = places[:, None] >= ends[None, :]
    return jnp.sum(before.astype(jnp.int32), axis=1)


def attend_kernel(with_output, with_grads, *refs):
    refs = list(refs)
    allowed_ref, q_ref, k_ref, v_ref, v_t_ref = refs[:5]
    del refs[:5]
    if with_grads:
        k_t_ref, g_ref = refs[:2]
        del refs[:2]
    o_ref = refs.pop(0)
    if with_grads:
        dq_ref, dk_ref, dv_ref = refs
    allowed = allowed_ref[...] > 0.0
    keys, values, values_t = (k_ref[0], v_ref[0], v_t_ref[...])
    dk = jnp.zeros(keys.shape, jnp.float32)
    dv = jnp.zeros(keys.shape, jnp.float32)
    by_last = (((1,), (1,)), ((), ()))
    for head in range(H // KV):
        rows = slice(head * DH, (head + 1) * DH)
        query = q_ref[rows, :]
        scores = jnp.dot(keys, query, preferred_element_type=jnp.float32) * DH ** (-0.5)
        scores = jnp.where(allowed, scores, MASKED)
        row_max = jnp.max(scores, axis=0, keepdims=True)
        log_total = row_max + jnp.log(
            jnp.sum(jnp.exp(scores - row_max), axis=0, keepdims=True)
        )
        weights = jnp.where(allowed, jnp.exp(scores - log_total), 0.0)
        weights_bf = weights.astype(jnp.bfloat16)
        if with_output:
            output = jnp.dot(values_t, weights_bf, preferred_element_type=jnp.float32)
            output = output.astype(jnp.bfloat16)
            o_ref[rows, :] = output
        else:
            output = o_ref[rows, :]
        if with_grads:
            grad = g_ref[rows, :]
            correction = jnp.sum(
                grad.astype(jnp.float32) * output.astype(jnp.float32), axis=0, keepdims=True
            )
            grad_weights = jnp.dot(values, grad, preferred_element_type=jnp.float32)
            grad_scores = (weights * (grad_weights - correction)).astype(jnp.bfloat16)
            grad_q = jnp.dot(k_t_ref[...], grad_scores, preferred_element_type=jnp.float32)
            dq_ref[rows, :] = (grad_q * DH ** (-0.5)).astype(jnp.bfloat16)
            dk += lax.dot_general(grad_scores, query, by_last, preferred_element_type=jnp.float32)
            dv += lax.dot_general(weights_bf, grad, by_last, preferred_element_type=jnp.float32)
    if with_grads:
        dk_ref[0] = dk
        dv_ref[0] = dv


def by_head(rows):
    return rows.reshape(rows.shape[0], KV, DH).transpose(1, 0, 2)


def from_heads(heads):
    return heads.transpose(1, 0, 2).reshape(heads.shape[1], KV * DH)


def attend(allowed_t, query_t, keys, values, output_t=None, grad_t=None):
    columns, rows = allowed_t.shape
    with_output, with_grads = (output_t is None, grad_t is not None)
    group = pl.BlockSpec((query_t.shape[0] // KV, rows), lambda g: (g, 0))
    key_rows = pl.BlockSpec((1, columns, DH), lambda g: (g, 0, 0))
    key_columns = pl.BlockSpec((DH, columns), lambda g: (g, 0))
    args = [allowed_t, query_t, by_head(keys), by_head(values), values.T]
    in_specs = [pl.BlockSpec((columns, rows), lambda g: (0, 0)), group]
    in_specs += [key_rows, key_rows, key_columns]
    out_shape, out_specs = ([], [])
    wide = jax.ShapeDtypeStruct(query_t.shape, jnp.bfloat16)
    narrow = jax.ShapeDtypeStruct((KV, columns, DH), jnp.float32)
    if with_grads:
        args += [keys.T, grad_t]
        in_specs += [key_columns, group]
    if with_output:
        out_shape.append(wide)
        out_specs.append(group)
    else:
        args.append(output_t)
        in_specs.append(group)
    if with_grads:
        out_shape += [wide, narrow, narrow]
        out_specs += [group, key_rows, key_rows]
    return pl.pallas_call(
        functools.partial(attend_kernel, with_output, with_grads),
        grid=(KV,),
        out_shape=tuple(out_shape),
        in_specs=in_specs,
        out_specs=tuple(out_specs),
    )(*args)


MESH = pl.DeviceIdType.MESH


def remote(src, dst, send_sem, recv_sem, ctx, fsdp):
    return pltpu.make_async_remote_copy(
        src_ref=src,
        dst_ref=dst,
        send_sem=send_sem,
        recv_sem=recv_sem,
        device_id={"ctx": ctx, "fsdp": fsdp},
        device_id_type=MESH,
    )


def place():
    return (lax.axis_index("ctx"), lax.axis_index("fsdp"))


def shard_at(z, core, planes, offset):
    return 2 * lax.rem(z + offset, planes) + core


def greet(planes):
    c, f = place()
    z, core = (f // 2, lax.rem(f, 2))
    barrier = pltpu.get_barrier_semaphore()
    peers = [(c ^ 1, f), (c ^ 2, f), (c ^ 3, f), (c, f ^ 1)]
    peers += [(c, shard_at(z, core, planes, d)) for d in range(1, planes)]
    for ctx, fsdp in peers:
        pl.semaphore_signal(
            barrier, inc=1, device_id={"ctx": ctx, "fsdp": fsdp}, device_id_type=MESH
        )
    pl.semaphore_wait(barrier, len(peers))


def quarter_of(ref, weight, quarter):
    if weight == 0:
        size = ref.shape[0] // 4
        return ref.at[pl.ds(pl.multiple_of(quarter * size, 16), size), :]
    size = ref.shape[1] // 4
    return ref.at[:, pl.ds(pl.multiple_of(quarter * size, 128), size)]


def by_distance(planes):
    order = []
    for step in range(1, planes // 2 + 1):
        for d in (step, planes - step):
            if d not in order:
                order.append(d)
    return order


def gather_kernel(
    planes, wo, wq, kv, go, gq, gkv, send, recv_z, recv_x, recv_y, recv_d, recv_p, recv_kv, local
):
    c, f = place()
    z, core = (f // 2, lax.rem(f, 2))
    mine, full = ((wo, wq), (go, gq))
    rows = kv.shape[0]
    owns = [
        pltpu.make_async_copy(kv, gkv.at[pl.ds(pl.multiple_of(c * rows, 128), rows)], local),
        pltpu.make_async_copy(wo, go.at[f], local),
        pltpu.make_async_copy(wq, gq.at[f], local),
    ]
    for copy in owns:
        copy.start()
    greet(planes)
    started = []

    def push(*args):
        copy = remote(*args)
        copy.start()
        started.append(copy)

    def piece(weight, shard, quarter):
        return quarter_of(full[weight].at[shard], weight, quarter)

    def arrive(ref, sem):
        remote(ref, ref, send, sem, c ^ 1, f).wait_recv()

    kv_place = gkv.at[pl.ds(pl.multiple_of(c * rows, 128), rows)]
    for i, bit in enumerate((1, 2, 3)):
        push(kv, kv_place, send, recv_kv.at[i], c ^ bit, f)
    order = by_distance(planes)
    for weight in (0, 1):
        for d in order:
            push(
                quarter_of(mine[weight], weight, c),
                piece(weight, f, c),
                send,
                recv_z.at[weight, d],
                c,
                shard_at(z, core, planes, d),
            )
        push(mine[weight], full[weight].at[f], send, recv_p.at[weight, 0, 0], c, f ^ 1)
    steps = [(weight, d) for weight in (0, 1) for d in order]

    def to_partner(weight, d, shard, slot):
        part = piece(weight, shard, c ^ slot)
        push(part, part, send, recv_p.at[weight, d, slot], c, f ^ 1)

    def first(weight, d):
        shard = shard_at(z, core, planes, planes - d)
        part = piece(weight, shard, c)
        arrive(part, recv_z.at[weight, d])
        push(part, part, send, recv_x.at[weight, d], c ^ 1, f)
        push(part, part, send, recv_y.at[weight, d], c ^ 2, f)
        to_partner(weight, d, shard, 0)

    def second(weight, d):
        shard = shard_at(z, core, planes, planes - d)
        arrive(piece(weight, shard, c ^ 1), recv_x.at[weight, d])
        arrive(piece(weight, shard, c ^ 2), recv_y.at[weight, d])
        bit = jnp.where(core == weight, 1, 2)
        part = piece(weight, shard, c ^ bit)
        push(part, part, send, recv_d.at[weight, d], c ^ (3 - bit), f)
        to_partner(weight, d, shard, 1)
        to_partner(weight, d, shard, 2)

    def third(weight, d):
        shard = shard_at(z, core, planes, planes - d)
        arrive(piece(weight, shard, c ^ 3), recv_d.at[weight, d])
        to_partner(weight, d, shard, 3)

    count = len(steps)
    for i in range(count + 2):
        if i < count:
            first(*steps[i])
        if 0 <= i - 1 < count:
            second(*steps[i - 1])
        if 0 <= i - 2 < count:
            third(*steps[i - 2])
    for weight in (0, 1):
        arrive(full[weight].at[f ^ 1], recv_p.at[weight, 0, 0])
        for d in order:
            shard = shard_at(z, core, planes, planes - d) ^ 1
            for slot in range(4):
                arrive(piece(weight, shard, c ^ slot), recv_p.at[weight, d, slot])
    for i in range(3):
        arrive(kv_place, recv_kv.at[i])
    for copy in started:
        copy.wait_send()
    for copy in owns:
        copy.wait()


def gather_weights(w_out, w_qkv, kv):
    count = lax.axis_size("fsdp")
    planes = count // 2
    dma = pltpu.SemaphoreType.DMA
    anywhere = pl.BlockSpec(memory_space=pl.ANY)
    return pl.pallas_call(
        functools.partial(gather_kernel, planes),
        out_shape=(
            jax.ShapeDtypeStruct((count,) + w_out.shape, w_out.dtype),
            jax.ShapeDtypeStruct((count,) + w_qkv.shape, w_qkv.dtype),
            jax.ShapeDtypeStruct((4 * kv.shape[0], kv.shape[1]), kv.dtype),
        ),
        in_specs=[anywhere] * 3,
        out_specs=(anywhere,) * 3,
        scratch_shapes=[
            dma,
            dma((2, planes)),
            dma((2, planes)),
            dma((2, planes)),
            dma((2, planes)),
            dma((2, planes, 4)),
            dma((3,)),
            dma,
        ],
        compiler_params=pltpu.CompilerParams(collective_id=0, has_side_effects=True),
    )(w_out, w_qkv, kv)


def reduce_kernel(
    planes,
    att_t,
    norm_t,
    grad_mid,
    grad_proj,
    kv_sums,
    out_o,
    out_q,
    out_kv,
    a_o,
    a_q,
    s_o,
    s_q,
    p_o,
    p_q,
    r1_o,
    r1_q,
    r2_o,
    r2_q,
    rz_o,
    rz_q,
    from_kv,
    send,
    recv_p,
    recv_1,
    recv_2,
    recv_z,
    recv_f,
    recv_kv,
):
    c, f = place()
    z, core = (f // 2, lax.rem(f, 2))
    greet(planes)
    own, sent, from_p, from_1, from_2, from_z, result = (
        (a_o, a_q),
        (s_o, s_q),
        (p_o, p_q),
        (r1_o, r1_q),
        (r2_o, r2_q),
        (rz_o, rz_q),
        (out_o, out_q),
    )
    started = []

    def push(*args):
        copy = remote(*args)
        copy.start()
        started.append(copy)

    def arrive(ref, sem):
        remote(ref, ref, send, sem, c ^ 1, f).wait_recv()

    def term(weight, shard):
        if weight == 0:
            size = a_o.shape[1]
            left = att_t[pl.ds(pl.multiple_of(shard * size, size), size), :]
            right = grad_mid[...]
        else:
            left = norm_t[shard]
            right = grad_proj[...]
        return jnp.dot(left, right, preferred_element_type=jnp.float32).astype(jnp.bfloat16)

    def added(first, second):
        return (first.astype(jnp.float32) + second.astype(jnp.float32)).astype(jnp.bfloat16)

    rows = out_kv.shape[0]

    def kv_rows(index):
        return kv_sums.at[pl.ds(pl.multiple_of(index * rows, rows), rows), :]

    for slot in (3, 1, 2):
        push(
            kv_rows(c ^ slot), from_kv.at[slot], send, recv_kv.at[slot], c ^ slot, f
        )
    order = by_distance(planes)[::-1] + [0]
    steps = [(weight, d) for d in order for weight in (1, 0)]

    def bits(weight):
        bit = jnp.where(core == weight, 1, 2)
        return (bit, 3 - bit)

    def produce(weight, d):
        shard = shard_at(z, core, planes, d)
        sent[weight][d] = term(weight, shard ^ 1)
        push(sent[weight].at[d], from_p[weight].at[d], send, recv_p.at[weight, d], c, f ^ 1)
        own[weight][d] = term(weight, shard)

    def chip_sum(weight, d):
        arrive(from_p[weight].at[d], recv_p.at[weight, d])
        own[weight][d] = added(own[weight][d], from_p[weight][d])
        bit, other = bits(weight)
        for slot, quarter in ((1, c ^ 3), (0, c ^ bit)):
            push(
                quarter_of(own[weight].at[d], weight, quarter),
                from_1[weight].at[d, slot],
                send,
                recv_1.at[weight, d, slot],
                c ^ bit,
                f,
            )

    def pair_sum(weight, d):
        bit, other = bits(weight)
        for slot, quarter in ((1, c ^ other), (0, c)):
            arrive(from_1[weight].at[d, slot], recv_1.at[weight, d, slot])
            part = quarter_of(own[weight].at[d], weight, quarter)
            part[...] = added(part[...], from_1[weight][d, slot])
            if slot == 1:
                push(part, from_2[weight].at[d], send, recv_2.at[weight, d], c ^ other, f)

    def plane_sum(weight, d):
        arrive(from_2[weight].at[d], recv_2.at[weight, d])
        part = quarter_of(own[weight].at[d], weight, c)
        part[...] = added(part[...], from_2[weight][d])
        if d:
            push(
                part,
                from_z[weight].at[d],
                send,
                recv_z.at[weight, d],
                c,
                shard_at(z, core, planes, d),
            )

    def finish(weight):
        part = quarter_of(own[weight].at[0], weight, c)
        total = part[...].astype(jnp.float32)
        for d in range(1, planes):
            arrive(from_z[weight].at[d], recv_z.at[weight, d])
            total = total + from_z[weight][d].astype(jnp.float32)
        place_c = quarter_of(result[weight], weight, c)
        place_c[...] = total.astype(jnp.bfloat16)
        for slot in (3, 1, 2):
            push(place_c, place_c, send, recv_f.at[weight, slot], c ^ slot, f)

    stages = (produce, chip_sum, pair_sum, plane_sum)
    lags = (0, 2, 4, 6)
    count = len(steps)
    for i in range(count + lags[-1]):
        for stage, lag in zip(stages, lags):
            if 0 <= i - lag < count:
                stage(*steps[i - lag])
    kv_total = kv_rows(c)[...].astype(jnp.float32)
    for slot in (1, 2, 3):
        arrive(from_kv.at[slot], recv_kv.at[slot])
        kv_total += from_kv[slot].astype(jnp.float32)
    out_kv[...] = kv_total
    for weight in (1, 0):
        finish(weight)
    for weight in (1, 0):
        for slot in (3, 1, 2):
            arrive(quarter_of(result[weight], weight, c ^ slot), recv_f.at[weight, slot])
    for copy in started:
        copy.wait_send()


def reduce_weights(att_t, norm_t, grad_mid, grad_proj, kv_sums):
    count = lax.axis_size("fsdp")
    planes = count // 2
    dma = pltpu.SemaphoreType.DMA
    in_vmem = pl.BlockSpec(memory_space=pltpu.VMEM)
    bf = jnp.bfloat16
    o_shape = (att_t.shape[0] // count, grad_mid.shape[1])
    q_shape = (norm_t.shape[1], grad_proj.shape[1])
    o_part = (o_shape[0] // 4, o_shape[1])
    q_part = (q_shape[0], q_shape[1] // 4)
    scratch = []
    for lead, shapes in (
        ((planes,), (o_shape, q_shape)),
        ((planes,), (o_shape, q_shape)),
        ((planes,), (o_shape, q_shape)),
        ((planes, 2), (o_part, q_part)),
        ((planes,), (o_part, q_part)),
        ((planes,), (o_part, q_part)),
    ):
        scratch += [pltpu.VMEM(lead + shape, bf) for shape in shapes]
    kv_shape = (kv_sums.shape[0] // 4, kv_sums.shape[1])
    scratch.append(pltpu.VMEM((4,) + kv_shape, bf))
    return pl.pallas_call(
        functools.partial(reduce_kernel, planes),
        out_shape=(
            jax.ShapeDtypeStruct(o_shape, bf),
            jax.ShapeDtypeStruct(q_shape, bf),
            jax.ShapeDtypeStruct(kv_shape, jnp.float32),
        ),
        in_specs=[in_vmem] * 5,
        out_specs=(in_vmem,) * 3,
        scratch_shapes=scratch
        + [
            dma,
            dma((2, planes)),
            dma((2, planes, 2)),
            dma((2, planes)),
            dma((2, planes)),
            dma((2, 4)),
            dma((4,)),
        ],
        compiler_params=pltpu.CompilerParams(
            collective_id=1, has_side_effects=True, vmem_limit_bytes=60 * 2**20
        ),
    )(att_t, norm_t, grad_mid, grad_proj, kv_sums)


def mega_kernel(
    planes,
    lens,
    q_in,
    k_in,
    v_in,
    resid_in,
    wo_in,
    wq_in,
    go_in,
    gr_in,
    out_b,
    out_gm,
    out_dq,
    out_dk,
    out_dv,
    res_a,
    res_b,
    res_q,
    q_v,
    resid_v,
    wo_v,
    go_v,
    gr_v,
    w_o,
    w_q,
    kv,
    kh,
    vh,
    kv_t,
    qp,
    gp,
    bias,
    bias_b,
    probs,
    o_p,
    att_t,
    att8,
    attq,
    acc,
    acc_p,
    normed,
    inv,
    xb,
    nt,
    kvx,
    khb,
    vhb,
    kvx_t,
    qb,
    ob_t,
    dqb_t,
    dkv_b,
    tail,
    head,
    gp4,
    gpq,
    gn,
    gm,
    dkv_t,
    kvs,
    kvr,
    s_q,
    p_q,
    o_q,
    z_q,
    t_q,
    s_a,
    p_a,
    o_a,
    z_a,
    t_a,
    s_b,
    p_b,
    o_b,
    z_b,
    t_b,
    local,
    send,
    recv_kv,
    recv_z,
    recv_x,
    recv_y,
    recv_d,
    recv_p,
    recv_att,
    recv_nt,
    recv_halo,
    recv_gp,
    recv_gm,
    recv_kvs,
    recv_rp,
    recv_rz,
    recv_rq,
    recv_f,
):
    f32, bf = (jnp.float32, jnp.bfloat16)
    c, f = place()
    z, core = (f // 2, lax.rem(f, 2))
    toks = q_in.shape[0]
    kvd = k_in.shape[1]
    shards = 2 * planes
    groups = kh.shape[0]
    pairs = qp.shape[0]
    per_group = pairs // groups
    per_shard = att_t.shape[1]
    scale = DH ** (-0.5)
    full = (w_o, w_q)
    by_last = (((1,), (1,)), ((), ()))
    started = []

    def push(*args, when=None):
        copy = remote(*args)
        if when is None:
            copy.start()
        else:
            pl.when(when)(copy.start)
        started.append((when, copy))

    def by_plane(table):
        return sum(jnp.where(z == i, entry, 0) for i, entry in enumerate(table))

    near = [sorted((s for s in range(planes) if s != i), key=lambda s: abs(s - i)) for i in range(planes)]
    sources = [by_plane(column) for column in zip(*near)]
    order = [
        sorted(
            (s for s in range(planes) if s != i),
            key=lambda s: (i if s > i else planes - 1 - i, -abs(s - i)),
        )
        for i in range(planes)
    ]
    targets = [by_plane(column) for column in zip(*order)]
    last = planes - 1
    edge = (z == 0) | (z == last)
    between = (z > 0) & (z < last)

    def arrive(ref, sem):
        remote(ref, ref, send, sem, c ^ 1, f).wait_recv()

    def dot(a, b):
        return jnp.dot(a, b, preferred_element_type=f32)

    def dot_nt(a, b):
        return lax.dot_general(a, b, by_last, preferred_element_type=f32)

    def share_rows(ref, sems):
        for bit in (1, 2):
            push(ref.at[c], ref.at[c], send, sems.at[bit], c ^ bit, f)

    def relay_rows(ref, sems):
        half = ref.shape[1] // 2
        for bit in (1, 2):
            arrive(ref.at[c ^ bit], sems.at[bit])
            part = ref.at[c ^ bit, pl.ds((bit - 1) * half, half)]
            push(part, part, send, sems.at[2 + bit], c ^ (3 - bit), f)

    def far_rows(ref, sems):
        half = ref.shape[1] // 2
        for bit in (1, 2):
            arrive(ref.at[c ^ 3, pl.ds((bit - 1) * half, half)], sems.at[2 + bit])

    names = ((wo_in, wo_v), (q_in, q_v), (resid_in, resid_v), (go_in, go_v), (gr_in, gr_v))
    loads = [
        pltpu.make_async_copy(src, dst, local.at[i]) for i, (src, dst) in enumerate(names)
    ]
    loads.append(pltpu.make_async_copy(k_in, kv.at[c, :, pl.ds(0, kvd)], local.at[5]))
    loads.append(pltpu.make_async_copy(v_in, kv.at[c, :, pl.ds(kvd, kvd)], local.at[6]))
    loads.append(pltpu.make_async_copy(wq_in, w_q.at[f], local.at[7]))
    for copy in loads:
        copy.start()
    greet(planes)
    for slot in (1, 2, 3):
        for i, src in enumerate((k_in, v_in)):
            push(
                src,
                kv.at[c, :, pl.ds(i * kvd, kvd)],
                send,
                recv_kv.at[slot, i],
                c ^ slot,
                f,
            )
    loads[0].wait()
    w_o[f] = wo_v[...].T
    slots = range(planes - 1)

    def piece(weight, shard, quarter):
        return quarter_of(full[weight].at[shard], weight, quarter)

    def share(weight):
        mine = w_o.at[f] if weight == 0 else wq_in
        for plane, ok in ((z + 1, z < last), (z - 1, z > 0)):
            push(
                quarter_of(mine, weight, c),
                piece(weight, f, c),
                send,
                recv_z.at[weight, z],
                c,
                2 * plane + core,
                when=ok,
            )
        push(mine, full[weight].at[f], send, recv_p.at[weight, 0, 0], c, f ^ 1)

    share(0)
    share(1)
    steps = [(weight, d) for weight in (0, 1) for d in slots]
    count = len(steps)

    def to_partner(weight, d, shard, slot):
        part = piece(weight, shard, c ^ slot)
        push(part, part, send, recv_p.at[weight, d + 1, slot], c, f ^ 1)

    def first(weight, d):
        source = sources[d]
        shard = 2 * source + core
        part = piece(weight, shard, c)
        arrive(part, recv_z.at[weight, source])
        onward = jnp.where(source < z, z < last, z > 0)
        plane = jnp.where(source < z, z + 1, z - 1)
        push(part, part, send, recv_z.at[weight, source], c, 2 * plane + core, when=onward)
        push(part, part, send, recv_x.at[weight, d], c ^ 1, f)
        push(part, part, send, recv_y.at[weight, d], c ^ 2, f)
        to_partner(weight, d, shard, 0)

    def second(weight, d):
        shard = 2 * sources[d] + core
        arrive(piece(weight, shard, c ^ 1), recv_x.at[weight, d])
        arrive(piece(weight, shard, c ^ 2), recv_y.at[weight, d])
        bit = jnp.where(core == weight, 1, 2)
        part = piece(weight, shard, c ^ bit)
        push(part, part, send, recv_d.at[weight, d], c ^ (3 - bit), f)
        to_partner(weight, d, shard, 1)
        to_partner(weight, d, shard, 2)

    def third(weight, d):
        shard = 2 * sources[d] + core
        arrive(piece(weight, shard, c ^ 3), recv_d.at[weight, d])
        to_partner(weight, d, shard, 3)

    def whole_plane(weight, d):
        shard = 2 * sources[d] + 1 - core
        for slot in range(4):
            arrive(piece(weight, shard, c ^ slot), recv_p.at[weight, d + 1, slot])

    def gather_step(i):
        if i < count:
            first(*steps[i])
        if 0 <= i - 1 < count:
            second(*steps[i - 1])
        if 0 <= i - 2 < count:
            third(*steps[i - 2])

    ends = [lens[0, 0]]
    for i in range(1, lens.shape[1]):
        ends.append(ends[-1] + lens[0, i])

    def document(places):
        number = jnp.zeros(places.shape, jnp.int32)
        for end in ends:
            number = number + (places >= end).astype(jnp.int32)
        return number

    def bias_of(length, first_place, reach):
        shape = (length, toks)
        columns = lax.broadcasted_iota(jnp.int32, shape, 0) + first_place
        rows = lax.broadcasted_iota(jnp.int32, shape, 1) + c * toks
        allowed = (document(columns) == document(rows)) & (columns <= rows)
        if reach:
            allowed = allowed & (columns > rows - reach) & (columns >= 0)
        part = jnp.where(allowed, 0.0, MASKED).astype(f32)
        return jnp.concatenate([part, part], axis=1)

    bias[...] = bias_of(kv.shape[0] * toks, 0, 0)
    bias_b[...] = bias_of(2 * toks, (c - 1) * toks, BAND)

    def paired(tile):
        return jnp.concatenate([tile[:DH], tile[DH:]], axis=1)

    def unpaired(wide):
        return jnp.concatenate([wide[:, :toks], wide[:, toks:]], axis=0)

    wide = 2 * DH

    def scaled(tile):
        return (tile.astype(f32) * scale).astype(bf)

    loads[1].wait()
    for i in range(pairs):
        qp[i] = scaled(paired(q_v[:, wide * i : wide * (i + 1)].T))
    for copy in loads[5:7]:
        copy.wait()
    for slot in (1, 2, 3):
        for i in range(2):
            arrive(kv.at[c ^ slot, :, pl.ds(i * kvd, kvd)], recv_kv.at[slot, i])

    def spread(source, keys_to, values_to, both_t):
        both = source[...].reshape(-1, 2 * kvd)
        for g in range(groups):
            keys_to[g] = both[:, DH * g : DH * (g + 1)]
            values_to[g] = both[:, kvd + DH * g : kvd + DH * (g + 1)]
        turned = both.T
        for g in range(2 * groups):
            both_t[g] = turned[DH * g : DH * (g + 1)]

    spread(kv, kh, vh, kv_t)

    def softmax(scores):
        top = jnp.max(scores, axis=0, keepdims=True)
        raised = jnp.exp(scores - top)
        total = jnp.sum(raised, axis=0, keepdims=True)
        return raised * (1.0 / total)

    def forward(g):
        for j in range(per_group):
            i = per_group * g + j
            weights = softmax(dot(kh[g], qp[i]) + bias[...]).astype(bf)
            probs[i] = weights
            output = dot(kv_t[groups + g], weights).astype(bf)
            o_p[i] = output
            att_t[i // per_shard, i % per_shard] = unpaired(output)

    for g in range(groups):
        gather_step(g)
        forward(g)
    attq[c] = att_t[:, c // 2, pl.ds(pl.multiple_of(lax.rem(c, 2) * DH, DH), DH), :]
    for s in range(shards):
        for j in range(per_shard):
            att8[s, :, wide * j : wide * (j + 1)] = att_t[s, j].T
    loads[2].wait()
    loads[3].wait()
    loads[4].wait()
    acc[...] = resid_v[...].astype(f32).T
    for i in range(pairs):
        gp[i] = paired(go_v[:, wide * i : wide * (i + 1)].T)

    def project(weight, shard):
        left = (att8, xb)[weight]
        return dot(left[shard], full[weight][shard]) + dot(left[shard ^ 1], full[weight][shard ^ 1])

    arrive(w_o.at[f ^ 1], recv_p.at[0, 0, 0])
    acc[...] += project(0, f)
    at = groups
    for d in slots:
        gather_step(at)
        at += 1
        whole_plane(0, d)
        acc[...] += project(0, 2 * sources[d] + core)
    resid = acc[...].astype(bf).astype(f32)
    inverse = lax.rsqrt(jnp.mean(resid * resid, axis=1, keepdims=True) + EPSILON)
    inv[...] = inverse
    values = resid * inverse
    normed[...] = values
    rows_q = w_q.shape[1]
    for s in range(shards):
        xb[s] = values[:, rows_q * s : rows_q * (s + 1)].astype(bf)
    loads[7].wait()
    arrive(w_q.at[f ^ 1], recv_p.at[1, 0, 0])
    acc_p[...] = project(1, f)
    for s in range(shards):
        nt[c, s] = xb[s].T
    for d in slots:
        if at < count + 2:
            gather_step(at)
            at += 1
        whole_plane(1, d)
        acc_p[...] += project(1, 2 * sources[d] + core)

    width = qb.shape[0] * wide
    kvx[1] = acc_p[:, width:].astype(bf)
    ahead, behind = (lax.rem(c + 1, 4), lax.rem(c + 3, 4))
    push(kvx.at[1], kvx.at[0], send, recv_halo.at[0], ahead, f)
    share_rows(nt, recv_nt)
    for slot in (1, 2, 3):
        peer = c ^ slot
        push(
            att_t.at[:, peer // 2, pl.ds(pl.multiple_of(lax.rem(peer, 2) * DH, DH), DH), :],
            attq.at[c],
            send,
            recv_att.at[slot],
            peer,
            f,
        )
    for i in range(pairs):
        qb[i] = scaled(paired(acc_p[:, wide * i : wide * (i + 1)].astype(bf).T))
    arrive(kvx.at[0], recv_halo.at[0])
    spread(kvx, khb, vhb, kvx_t)

    def banded(g, carry):
        dk = jnp.zeros((DH, 2 * toks), f32)
        dv = jnp.zeros((DH, 2 * toks), f32)
        for j in range(per_group):
            i = per_group * g + j
            weights = softmax(dot(khb[g], qb[i]) + bias_b[...])
            weights_bf = weights.astype(bf)
            output = dot(kvx_t[groups + g], weights_bf).astype(bf)
            ob_t[i] = unpaired(output)
            grad = gp[i]
            correction = jnp.sum(grad.astype(f32) * output.astype(f32), axis=0, keepdims=True)
            grad_scores = (weights * (dot(vhb[g], grad) - correction)).astype(bf)
            dqb_t[i] = unpaired((dot(kvx_t[g], grad_scores) * scale).astype(bf))
            dk += dot_nt(qb[i], grad_scores)
            dv += dot_nt(grad, weights_bf)
        dkv_b[g] = dk
        dkv_b[groups + g] = dv
        return carry

    lax.fori_loop(0, groups, banded, 0)
    for g in range(2 * groups):
        tail[DH * g : DH * (g + 1)] = dkv_b[g, :, :toks].astype(bf)
    push(tail, head, send, recv_halo.at[1], behind, f)
    relay_rows(nt, recv_nt)
    gp_width = gp4.shape[2]

    def put_gp(column, block):
        gp4[column // gp_width, :, column % gp_width : column % gp_width + block.shape[1]] = block

    for i in range(pairs):
        out_b[:, wide * i : wide * (i + 1)] = ob_t[i].T
        put_gp(wide * i, dqb_t[i].T)
    arrive(head, recv_halo.at[1])
    own = jnp.concatenate([dkv_b[g, :, toks:] for g in range(2 * groups)], axis=0)
    own = (own + head[...].astype(f32)).astype(bf)
    for i in range(2 * groups * DH // wide):
        put_gp(width + wide * i, own[wide * i : wide * (i + 1)].T)
    for slot in (1, 2, 3):
        push(gp4.at[c ^ slot], gpq.at[c], send, recv_gp.at[slot], c ^ slot, f)
    gpq[c] = gp4[c]

    for s in range(shards):
        total = dot_nt(gp4[0], w_q[s, :, :gp_width])
        for b in range(1, 4):
            total += dot_nt(gp4[b], w_q[s, :, gp_width * b : gp_width * (b + 1)])
        gn[:, rows_q * s : rows_q * (s + 1)] = total
    middle = jnp.mean(gn[...] * normed[...], axis=1, keepdims=True)
    change = inv[...] * (gn[...] - normed[...] * middle)
    grad_mid = gr_v[...].astype(f32).T + change
    gm[c] = grad_mid.astype(bf)
    share_rows(gm, recv_gm)
    out_gm[...] = gm[c].T

    def sum_chip(weight, produce, sent, from_p, totals):
        for d in range(planes):
            sent[d] = produce(2 * d + 1 - core).astype(bf)
            push(sent.at[d], from_p.at[d], send, recv_rp.at[weight, d], c, f ^ 1)
        for d in range(planes):
            mine = produce(2 * d + core)
            arrive(from_p.at[d], recv_rp.at[weight, d])
            totals[d] = mine + from_p[d].astype(f32)

    def spread_result(weight, value, result):
        result[c] = value.astype(bf)
        for slot in (3, 1, 2):
            push(result.at[c], result.at[c], send, recv_f.at[weight, slot], c ^ slot, f)

    def onward(weight, slot, out, moving, ok):
        target = targets[slot]
        way = jnp.where(target > z, 0, 1)
        plane = jnp.where(target > z, z + 1, z - 1)
        push(
            out.at[slot],
            moving.at[way, target],
            send,
            recv_rz.at[weight, way, target],
            c,
            2 * plane + core,
            when=ok,
        )

    def direct(totals, out, moving):
        for slot in slots:
            target = sources[::-1][slot]
            out[slot] = totals[target].astype(bf)
            push(
                out.at[slot],
                moving.at[0, z],
                send,
                recv_rq.at[z],
                c,
                2 * target + core,
            )

    def finish_direct(totals, moving, result):
        value = totals[z]
        for source in sources:
            arrive(moving.at[0, source], recv_rq.at[source])
            value += moving[0, source].astype(f32)
        spread_result(1, value, result)

    def ends_send(weight, send_slots, totals, out, moving):
        for slot in send_slots:

            @pl.when(edge)
            def _():
                out[slot] = totals[targets[slot]].astype(bf)

            onward(weight, slot, out, moving, edge)

    def chain(weight, slot, totals, out, moving):
        target = targets[slot]
        way = jnp.where(target > z, 0, 1)

        @pl.when(between)
        def _():
            arrive(moving.at[way, target], recv_rz.at[weight, way, target])
            out[slot] = (totals[target] + moving[way, target].astype(f32)).astype(bf)

        onward(weight, slot, out, moving, between)

    def finish(weight, totals, moving, result):
        for way, ok in ((0, z > 0), (1, z < last)):

            @pl.when(ok)
            def _():
                arrive(moving.at[way, z], recv_rz.at[weight, way, z])
                totals[z] += moving[way, z].astype(f32)

        spread_result(weight, totals[z], result)

    def produce_q(shard):
        left = jnp.concatenate([nt[b, shard] for b in range(4)], axis=1)
        return dot(left, gpq[...].reshape(-1, gp_width))

    def produce_o(low, high, shard):
        left = jnp.concatenate([attq[b, shard] for b in range(4)], axis=1)
        return dot(left, gm[:, :, low:high].reshape(-1, high - low))

    split = res_a.shape[2]
    produce_a = functools.partial(produce_o, 0, split)
    produce_b = functools.partial(produce_o, split, gm.shape[2])
    for_q = (t_q, o_q, z_q)
    for_a = (t_a, o_a, z_a)
    for_b = (t_b, o_b, z_b)

    for s in range(shards):
        part = dot(w_o[s], out_gm[...]).astype(bf)
        for j in range(per_shard):
            gp[per_shard * s + j] = paired(part[wide * j : wide * (j + 1)])
    def backward(g, carry):
        dk = jnp.zeros((DH, 4 * toks), f32)
        dv = jnp.zeros((DH, 4 * toks), f32)
        for j in range(per_group):
            i = per_group * g + j
            grad, weights = (gp[i], probs[i])
            correction = jnp.sum(grad.astype(f32) * o_p[i].astype(f32), axis=0, keepdims=True)
            change = dot(vh[g], grad) - correction
            grad_scores = (weights.astype(f32) * change).astype(bf)
            dqb_t[i] = unpaired((dot(kv_t[g], grad_scores) * scale).astype(bf))
            dk += dot_nt(qp[i], grad_scores)
            dv += dot_nt(grad, weights)
        dkv_t[g] = dk
        dkv_t[groups + g] = dv
        return carry

    lax.fori_loop(0, groups // 2, backward, 0)
    far_rows(nt, recv_nt)
    for slot in (1, 2, 3):
        arrive(gpq.at[c ^ slot], recv_gp.at[slot])
    sum_chip(1, produce_q, s_q, p_q, t_q)
    direct(*for_q)
    relay_rows(gm, recv_gm)
    lax.fori_loop(groups // 2, groups, backward, 0)
    for b in range(4):
        for g in range(2 * groups):
            kvs[b, DH * g : DH * (g + 1)] = dkv_t[g, :, toks * b : toks * (b + 1)].astype(bf)
    for slot in (1, 2, 3):
        push(kvs.at[c ^ slot], kvr.at[slot], send, recv_kvs.at[slot], c ^ slot, f)
    for slot in (1, 2, 3):
        arrive(attq.at[c ^ slot], recv_att.at[slot])
    far_rows(gm, recv_gm)
    sum_chip(0, produce_a, s_a, p_a, t_a)
    ends_send(0, slots[:1], *for_a)
    sum_chip(2, produce_b, s_b, p_b, t_b)
    for slot in slots:
        if slot:
            ends_send(0, slots[slot : slot + 1], *for_a)
        ends_send(2, slots[slot : slot + 1], *for_b)
    for i in range(pairs):
        out_dq[:, wide * i : wide * (i + 1)] = dqb_t[i].T
    finish_direct(t_q, z_q, res_q)
    chain(0, 0, *for_a)
    chain(2, 0, *for_b)
    for slot in slots[1:]:
        chain(0, slot, *for_a)
        chain(2, slot, *for_b)
    total = kvs[c].astype(f32)
    for slot in (1, 2, 3):
        arrive(kvr.at[slot], recv_kvs.at[slot])
        total += kvr[slot].astype(f32)
    total = total.astype(bf).T
    out_dk[...] = total[:, :kvd]
    out_dv[...] = total[:, kvd:]
    finish(0, t_a, z_a, res_a)
    finish(2, t_b, z_b, res_b)
    for weight, result in ((1, res_q), (0, res_a), (2, res_b)):
        for slot in (3, 1, 2):
            arrive(result.at[c ^ slot], recv_f.at[weight, slot])
    for when, copy in started:
        if when is None:
            copy.wait_send()
        else:
            pl.when(when)(copy.wait_send)


def finish_kernel(b_in, gm_in, dq_in, dk_in, dv_in, oa, ob, q_in, b, gm, dq, dk, dv, wo, wq):
    for src, dst in ((b_in, b), (gm_in, gm), (dq_in, dq), (dk_in, dk), (dv_in, dv)):
        dst[...] = src[...]
    width = q_in.shape[2]
    for quarter in range(4):
        wq[:, width * quarter : width * (quarter + 1)] = q_in[quarter].astype(jnp.float32)
    split = oa.shape[2]
    wo[:split] = oa[...].reshape(-1, split).astype(jnp.float32).T
    wo[split:] = ob[...].reshape(-1, ob.shape[2]).astype(jnp.float32).T


def one_kernel(lengths, query, keys, values, resid, w_out, w_qkv, grad_out, grad_resid):
    shards = lax.axis_size("fsdp")
    planes = shards // 2
    bf, f32 = (jnp.bfloat16, jnp.float32)
    toks, hd = query.shape
    kvd = keys.shape[1]
    dim = resid.shape[1]
    rows_o, rows_q = (w_out.shape[0], w_qkv.shape[0])
    width = w_qkv.shape[1]
    wide = 2 * DH
    pairs = hd // wide
    groups = kvd // DH
    seq = 4 * toks
    shape = jax.ShapeDtypeStruct
    split = (dim // 256 + 1) * 128
    a_part, b_part = ((rows_o // 4, split), (rows_o // 4, dim - split))
    q_part = (rows_q, width // 4)
    outs = (
        shape((toks, hd), bf),
        shape((dim, toks), bf),
        shape((toks, hd), bf),
        shape((toks, kvd), bf),
        shape((toks, kvd), bf),
        shape((4,) + a_part, bf),
        shape((4,) + b_part, bf),
        shape((4,) + q_part, bf),
    )
    v = pltpu.VMEM
    scratch = [
        v((toks, hd), bf),
        v((dim, toks), bf),
        v((dim, rows_o), bf),
        v((toks, hd), bf),
        v((dim, toks), bf),
        v((shards, rows_o, dim), bf),
        v((shards, rows_q, width), bf),
        v((4, toks, 2 * kvd), bf),
        v((groups, seq, DH), bf),
        v((groups, seq, DH), bf),
        v((2 * groups, DH, seq), bf),
        v((pairs, DH, 2 * toks), bf),
        v((pairs, DH, 2 * toks), bf),
        v((seq, 2 * toks), f32),
        v((2 * toks, 2 * toks), f32),
        v((pairs, seq, 2 * toks), bf),
        v((pairs, DH, 2 * toks), bf),
        v((shards, rows_o // wide, wide, toks), bf),
        v((shards, toks, rows_o), bf),
        v((4, shards, rows_o // 4, toks), bf),
        v((toks, dim), f32),
        v((toks, width), f32),
        v((toks, dim), f32),
        v((toks, 1), f32),
        v((shards, toks, rows_q), bf),
        v((4, shards, rows_q, toks), bf),
        v((2, toks, 2 * kvd), bf),
        v((groups, 2 * toks, DH), bf),
        v((groups, 2 * toks, DH), bf),
        v((2 * groups, DH, 2 * toks), bf),
        v((pairs, DH, 2 * toks), bf),
        v((pairs, wide, toks), bf),
        v((pairs, wide, toks), bf),
        v((2 * groups, DH, 2 * toks), f32),
        v((2 * kvd, toks), bf),
        v((2 * kvd, toks), bf),
        v((4, toks, width // 4), bf),
        v((4, toks, width // 4), bf),
        v((toks, dim), f32),
        v((4, toks, dim), bf),
        v((2 * groups, DH, seq), f32),
        v((4, 2 * kvd, toks), bf),
        v((4, 2 * kvd, toks), bf),
    ]
    for part in (q_part, a_part, b_part):
        scratch += [
            v((planes,) + part, bf),
            v((planes,) + part, bf),
            v((planes,) + part, bf),
            v((2, planes) + part, bf),
            v((planes,) + part, f32),
        ]
    dma = pltpu.SemaphoreType.DMA
    scratch += [
        dma((8,)),
        dma,
        dma((4, 2)),
        dma((2, planes)),
        dma((2, planes)),
        dma((2, planes)),
        dma((2, planes)),
        dma((2, planes, 4)),
        dma((4,)),
        dma((5,)),
        dma((2,)),
        dma((4,)),
        dma((5,)),
        dma((4,)),
        dma((3, planes)),
        dma((3, 2, planes)),
        dma((planes,)),
        dma((3, 4)),
    ]
    anywhere = pl.BlockSpec(memory_space=pl.ANY)
    in_vmem = pl.BlockSpec(memory_space=pltpu.VMEM)
    results = pl.pallas_call(
        functools.partial(mega_kernel, planes),
        out_shape=outs,
        in_specs=[pl.BlockSpec(memory_space=pltpu.SMEM)] + [anywhere] * 8,
        out_specs=(in_vmem,) * 8,
        scratch_shapes=scratch,
        compiler_params=pltpu.CompilerParams(
            collective_id=0, has_side_effects=True, vmem_limit_bytes=60 * 2**20
        ),
    )(lengths, query, keys, values, resid.T, w_out.T, w_qkv, grad_out, grad_resid.T)
    final = outs[:5] + (shape((dim, rows_o), f32), shape((rows_q, width), f32))
    b, gm, dq, dk, dv, wo, wq = pl.pallas_call(
        finish_kernel,
        out_shape=final,
        in_specs=[in_vmem] * 8,
        out_specs=(in_vmem,) * 7,
    )(*results)
    return (b[None], gm.T[None], dq[None], dk[None], dv[None], wo.T, wq)


def per_device(query_a, key_a, value_a, resid_in, doc_lengths, w_out, w_qkv, grad_out, grad_resid):
    ctx_count = lax.axis_size("ctx")
    ctx_index = lax.axis_index("ctx")
    local_rows = query_a.shape[1]
    seq_len = local_rows * ctx_count
    band_len = BAND
    first_row = ctx_index * local_rows
    documents = doc_table(doc_lengths[0], seq_len)
    fsdp_count = lax.axis_size("fsdp")
    own_kernels = ctx_count == 4 and fsdp_count % 2 == 0 and w_out.shape[0] % 64 == 0
    if own_kernels and local_rows == BAND and w_out.shape[0] == 4 * DH and fsdp_count == 8:
        return one_kernel(
            doc_lengths,
            query_a[0],
            key_a[0],
            value_a[0],
            resid_in[0],
            w_out,
            w_qkv,
            grad_out[0],
            grad_resid[0],
        )
    if own_kernels:
        w_o3, w_b3, kv = gather_weights(
            w_out, w_qkv, jnp.concatenate([key_a[0], value_a[0]], axis=1)
        )
        w_o = w_o3.reshape(-1, w_out.shape[1])
        w_b = w_b3.reshape(-1, w_qkv.shape[1])
        keys, values = (kv[:, : KV * DH], kv[:, KV * DH :])
    else:
        w_o, w_b = (
            lax.all_gather(w_out, "fsdp", axis=0, tiled=True),
            lax.all_gather(w_qkv, "fsdp", axis=0, tiled=True),
        )
        keys, values = (
            lax.all_gather(key_a[0], "ctx", axis=0, tiled=True),
            lax.all_gather(value_a[0], "ctx", axis=0, tiled=True),
        )
    query_t = query_a[0].T
    row_docs = lax.dynamic_slice_in_dim(documents, first_row, local_rows)[None, :]
    row_places = (first_row + jnp.arange(local_rows, dtype=jnp.int32))[None, :]
    columns = jnp.arange(seq_len, dtype=jnp.int32)[:, None]
    allowed_t = ((documents[:, None] == row_docs) & (columns <= row_places)).astype(jnp.float32)
    (attended_t,) = attend(allowed_t, query_t, keys, values)
    attended = attended_t.T
    resid_mid = (
        resid_in[0].astype(jnp.float32) + jnp.dot(attended, w_o, preferred_element_type=jnp.float32)
    ).astype(jnp.bfloat16)
    resid_f = resid_mid.astype(jnp.float32)
    inverse_rms = lax.rsqrt(jnp.mean(resid_f * resid_f, axis=-1, keepdims=True) + EPSILON)
    normed = resid_f * inverse_rms
    normed_bf = normed.astype(jnp.bfloat16)
    projected = jnp.dot(normed_bf, w_b, preferred_element_type=jnp.float32).astype(jnp.bfloat16)
    query_b = projected[:, : H * DH]
    key_b = projected[:, H * DH : H * DH + KV * DH]
    value_b = projected[:, H * DH + KV * DH :]
    tails = from_behind(projected[:, H * DH :], "ctx", 1)
    tail_keys, tail_values = (tails[:, : KV * DH], tails[:, KV * DH :])
    keys_ext = jnp.concatenate([tail_keys, key_b], axis=0)
    values_ext = jnp.concatenate([tail_values, value_b], axis=0)
    doc_pad = jnp.concatenate([jnp.full((band_len,), -1, jnp.int32), documents])
    doc_ext = lax.dynamic_slice_in_dim(doc_pad, first_row, band_len + local_rows)
    ext_places = first_row - band_len + jnp.arange(band_len + local_rows, dtype=jnp.int32)
    ext_places = ext_places[:, None]
    band_t = (doc_ext[:, None] == row_docs) & (ext_places <= row_places)
    band_t = (band_t & (ext_places > row_places - band_len)).astype(jnp.float32)
    banded_t, grad_qb_t, key_heads, value_heads = attend(
        band_t, query_b.T, keys_ext, values_ext, None, grad_out[0].T
    )
    banded, grad_qb = (banded_t.T, grad_qb_t.T)
    key_ext_grad, value_ext_grad = (from_heads(key_heads), from_heads(value_heads))
    heads = jnp.concatenate([key_ext_grad[:band_len], value_ext_grad[:band_len]], axis=1)
    heads = from_behind(heads.astype(jnp.bfloat16), "ctx", -1).astype(jnp.float32)
    head_keys, head_values = (heads[:, : KV * DH], heads[:, KV * DH :])
    grad_kb = key_ext_grad[band_len:].at[local_rows - band_len :].add(head_keys)
    grad_vb = value_ext_grad[band_len:].at[local_rows - band_len :].add(head_values)
    grad_kb = (grad_kb * DH ** (-0.5)).astype(jnp.bfloat16)
    grad_vb = grad_vb.astype(jnp.bfloat16)
    grad_proj = jnp.concatenate([grad_qb, grad_kb, grad_vb], axis=1)
    grad_normed = jnp.dot(grad_proj, w_b.T, preferred_element_type=jnp.float32)
    middle = jnp.mean(grad_normed * normed, axis=-1, keepdims=True)
    grad_mid = (
        grad_resid[0].astype(jnp.float32) + inverse_rms * (grad_normed - normed * middle)
    ).astype(jnp.bfloat16)
    grad_attended = jnp.dot(grad_mid, w_o.T, preferred_element_type=jnp.float32).astype(
        jnp.bfloat16
    )
    grad_query_t, key_heads, value_heads = attend(
        allowed_t, query_t, keys, values, attended_t, grad_attended.T
    )
    grad_query = grad_query_t.T
    key_sums, value_sums = (from_heads(key_heads), from_heads(value_heads))
    if own_kernels:
        norm_t = normed_bf.T.reshape(fsdp_count, -1, local_rows)
        kv_sums = jnp.concatenate([key_sums, value_sums], axis=1).astype(jnp.bfloat16)
        out_share, qkv_share, own_kv = reduce_weights(
            attended_t, norm_t, grad_mid, grad_proj, kv_sums
        )
        own_keys, own_values = (own_kv[:, : KV * DH], own_kv[:, KV * DH :])
        grad_w_out, grad_w_qkv = (out_share.astype(jnp.float32), qkv_share.astype(jnp.float32))
    else:
        own_keys, own_values = (
            lax.psum_scatter(
                key_sums.astype(jnp.bfloat16), "ctx", scatter_dimension=0, tiled=True
            ).astype(jnp.float32),
            lax.psum_scatter(
                value_sums.astype(jnp.bfloat16), "ctx", scatter_dimension=0, tiled=True
            ).astype(jnp.float32),
        )
        piece = normed_bf
        qkv_share = lax.psum_scatter(
            jnp.einsum("tf,tc->fc", piece, grad_proj, preferred_element_type=jnp.float32).astype(
                jnp.bfloat16
            ),
            "fsdp",
            scatter_dimension=0,
            tiled=True,
        )
        piece = attended
        out_share = lax.psum_scatter(
            jnp.einsum("tf,tc->fc", piece, grad_mid, preferred_element_type=jnp.float32).astype(
                jnp.bfloat16
            ),
            "fsdp",
            scatter_dimension=0,
            tiled=True,
        )
        grad_w_out, grad_w_qkv = (
            lax.psum(out_share, "ctx").astype(jnp.float32),
            lax.psum(qkv_share, "ctx").astype(jnp.float32),
        )
    grad_key = (own_keys * DH ** (-0.5)).astype(jnp.bfloat16)
    grad_value = own_values.astype(jnp.bfloat16)
    return (
        banded[None],
        grad_mid[None],
        grad_query[None],
        grad_key[None],
        grad_value[None],
        grad_w_out,
        grad_w_qkv,
    )


def solution(mesh):
    in_specs = (
        P("fsdp", "ctx", None),
        P("fsdp", "ctx", None),
        P("fsdp", "ctx", None),
        P("fsdp", "ctx", None),
        P("fsdp", None),
        P("fsdp", None),
        P("fsdp", None),
        P("fsdp", "ctx", None),
        P("fsdp", "ctx", None),
    )
    out_specs = (
        P("fsdp", "ctx", None),
        P("fsdp", "ctx", None),
        P("fsdp", "ctx", None),
        P("fsdp", "ctx", None),
        P("fsdp", "ctx", None),
        P("fsdp", None),
        P("fsdp", None),
    )
    return jax.shard_map(
        per_device, mesh=mesh, in_specs=in_specs, out_specs=out_specs, check_vma=False
    )
```
